128 devices in a mesh: plane: 8 (over z_hi, x), tile: 16 (over z_lo, y, core).
Axes of the slice: x: 4, y: 4, z: 4 (z_hi: 2, z_lo: 2; z = z_hi * 2 + z_lo), core: 2. Of those that a mesh axis runs over, the one named last changes fastest.
Arguments:
- visibility: float32 [2, 262144], P(None, ('plane', 'tile')), may hold values from -6 to 6
- target: int32 [262144, 1], P(('plane', 'tile')), may hold values from 0 to 127; in each aligned block of 2048 rows (0 to 2047, 2048 to 4095, ...) at most 32 rows name the same one
- offset: int32 [262144], P(('plane', 'tile')), may hold values from 0 to 1048575
- taps: float32 [8], replicated, may hold values from 0.1 to 1
- w_plane: float32 [8], P('plane'), may hold values from -300 to 300
Outputs:
- dirty_image: float32 [4096, 4096], P('plane', 'tile')
The draws below stay inside these ranges and needn't reach their ends.
Inputs may be any that keep to these rules, and one draw needn't show every extreme that they name: `target`: among the rows of one device no value occurs more than 32 times, and some value occurs exactly 32 times.
All inputs are finite; a program needn't handle non-finite values.
Results may differ from the reference program's by a relative error of at most 0.0042.
Values sent between devices are 32-bit elements; how exact they have to be, the bound alone decides.
No kernel may reach another device: no remote copies, remote signals or barrier semaphores. Data moves between devices by JAX's collectives and lax.ppermute only.
A program may use at most 128 MiB of HBM per device.

```python
import math
import jax
import jax.numpy as jnp
import numpy as np
from jax import lax

G = 4096
KS = 8
VIS_DEV = 2048
PLANES = 8
ROWS = 256
CAP = 32
VIS_ALL = 262144
N_PLANE = 8
N_TILE = 16


def plant(entries, key, smallest, largest):
    spot = [jax.random.randint(jax.random.fold_in(key, axis), (), 0, length) for axis, length in enumerate(entries.shape)]
    main_axis = entries.shape.index(max(entries.shape))
    neighbour = spot[:main_axis] + [(spot[main_axis] + 1) % entries.shape[main_axis]] + spot[main_axis + 1:]
    return entries.at[tuple(spot)].set(smallest).at[tuple(neighbour)].set(largest)


def shard_levels(own_key, shape, pieces, low, largest):
    level = 1.0
    for dim, parts in pieces:
        draws = jax.random.uniform(jax.random.fold_in(jax.random.fold_in(own_key, 6), dim), (parts,), jnp.float32, low / len(pieces), largest / len(pieces))
        level = level * jnp.repeat(jnp.exp(draws), shape[dim] // parts).reshape((-1,) + (1,) * (len(shape) - 1 - dim))
    return level


def deal_out(key, own, number, rows, count, top, reach, lean):
    sequence = jax.random.permutation(key, count)
    packed, common = load_shares(count, rows * top, reach, lean, True), load_shares(count, rows * top, reach, lean, False)
    places = jnp.arange(count)

    def named(sizes, rotation):
        used = int((sizes > 0).sum())
        fixed = max(1, used // 4)
        shifted = fixed + (places - fixed + rotation * (used - fixed)) % max(1, count - fixed)
        return jnp.zeros((count,), jnp.int32).at[sequence[jnp.where(places < fixed, places, shifted)]].set(jnp.asarray(sizes, jnp.int32))

    sizes = jnp.where(number % 4 == 0, named(packed, number // 4), named(common, number - number // 4 - 1))
    mixed = jax.random.permutation(jax.random.fold_in(own, 3), count)
    donor, receiver = mixed[0:count // 2 * 2:2], mixed[1:count // 2 * 2:2]
    slack = jnp.minimum(sizes[donor] - 1, reach - sizes[receiver]) // 2
    slack = jnp.where((donor == sequence[0]) | (receiver == sequence[0]) | (sizes[receiver] == 0), 0, jnp.maximum(slack, 0))
    shifted = jax.random.randint(jax.random.fold_in(own, 4), (count // 2,), 0, 1 << 20) % (slack + 1)
    sizes = sizes.at[donor].add(-shifted).at[receiver].add(shifted)
    members = jnp.searchsorted(jnp.cumsum(sizes), jnp.arange(rows * top), side="right").astype(jnp.int32)
    grid = members.reshape(top, rows).T
    grid = grid[jax.random.permutation(jax.random.fold_in(own, 1), rows)]
    rotation = jax.random.randint(jax.random.fold_in(own, 2), (rows, 1), 0, top)
    return jnp.take_along_axis(grid, (jnp.arange(top)[None, :] + rotation) % top, axis=1)


def load_shares(number_of, total, limit, skew, full):
    weights = [(1 << 20) // math.isqrt(grade ** skew) + 1 for grade in range(1, number_of + 1)]
    largest = limit if full else min(limit, max(-(-total // number_of), total * weights[0] // sum(weights)))
    least = 1 if total - largest >= number_of - 1 else 0
    holding, spare = [largest] + [least] * (number_of - 1), total - largest - least * (number_of - 1)
    while spare > 0:
        free = [i for i in range(1, number_of) if holding[i] < largest] or [i for i in range(1, number_of) if holding[i] < limit]
        pool, budget = sum([weights[i] for i in free]), spare
        for i in free:
            more = min(limit - holding[i], max(1, budget * weights[i] // pool), spare)
            holding[i] = holding[i] + more
            spare = spare - more
    return np.array(holding)


def gaussian(rng, shape, deviation, most, shards=(), kind=jnp.bfloat16):
    result = deviation * jax.random.normal(rng, shape, jnp.float32)
    if shards:
        result = result * shard_levels(rng, shape, shards, -0.22, 0.18)
    return jnp.clip(result, -most, most).astype(kind)


def setup_inputs(seed: int = 0) -> dict:
    keys = jax.random.split(jax.random.key(seed), 6)
    visibility = gaussian(keys[0], (2, VIS_ALL), 1.0, 6.0, ((1, 128),), jnp.float32)
    target_keys = jax.random.split(jax.random.fold_in(keys[1], 1), VIS_ALL // VIS_DEV)
    target_turns = jax.random.permutation(jax.random.fold_in(keys[1], 3), VIS_ALL // VIS_DEV)
    target = jax.vmap(lambda own, number: deal_out(jax.random.fold_in(keys[1], 2), own, number, VIS_DEV, N_PLANE * N_TILE, 1, CAP, 2))(target_keys, target_turns).reshape((VIS_ALL, 1))
    offset = plant(jax.random.randint(keys[2], (VIS_ALL,), 0, ROWS * G), jax.random.fold_in(keys[2], 1), 0, (ROWS * G) - 1).astype(jnp.int32)
    taps = jnp.clip(jnp.exp(jax.random.uniform(keys[3], (KS,), jnp.float32, math.log(0.1), math.log(1.0))), 0.1, 1.0)
    w_plane = jnp.clip(jax.random.uniform(keys[4], (PLANES,), jnp.float32, -300.0, 300.0) * shard_levels(keys[4], (PLANES,), ((0, 8),), -0.4, 0.0), -300.0, 300.0)
    return dict(visibility=visibility, target=target, offset=offset, taps=taps, w_plane=w_plane)


def direction(index, length):
    return ((index + length // 2) % length - length // 2).astype(jnp.float32) * (0.5 / length)

def reference(visibility, target, offset, taps, w_plane):
    destination = target[:, 0]
    plane_of = destination // N_TILE
    tile_of = destination % N_TILE
    grid_row = tile_of * (G // N_TILE) + offset // G
    grid_col = offset % G
    kernel_len = taps.shape[0]
    count = visibility.shape[1]
    weight_re = lax.optimization_barrier((taps[None, :] * visibility[0][:, None]).astype(jnp.bfloat16)).astype(jnp.float32)
    weight_im = lax.optimization_barrier((taps[None, :] * visibility[1][:, None]).astype(jnp.bfloat16)).astype(jnp.float32)
    taps_round = lax.optimization_barrier(taps.astype(jnp.bfloat16)).astype(jnp.float32)
    shifts = jnp.arange(kernel_len, dtype=jnp.int32)
    row_index = (grid_row[:, None] + shifts[None, :]) % G
    col_index = (grid_col[:, None] + shifts[None, :]) % G
    row_full = jnp.broadcast_to(row_index[:, :, None], (count, kernel_len, kernel_len))
    col_full = jnp.broadcast_to(col_index[:, None, :], (count, kernel_len, kernel_len))
    lines = jnp.arange(G, dtype=jnp.int32)
    cosines = direction(lines, G)
    n_minus = jnp.sqrt(1.0 - cosines[:, None] * cosines[:, None] - cosines[None, :] * cosines[None, :]) - 1.0
    image = jnp.zeros((G, G), jnp.float32)
    for plane in range(N_PLANE):
        mask = (plane_of == plane).astype(jnp.float32)
        value_re = (weight_re * mask[:, None])[:, :, None] * taps_round[None, None, :]
        value_im = (weight_im * mask[:, None])[:, :, None] * taps_round[None, None, :]
        grid_re = jnp.zeros((G, G), jnp.float32).at[row_full, col_full].add(value_re)
        grid_im = jnp.zeros((G, G), jnp.float32).at[row_full, col_full].add(value_im)
        transformed = jnp.fft.ifft2(grid_re + 1j * grid_im) * (G * G)
        phase = 2.0 * math.pi * w_plane[plane] * n_minus
        image = image + (jnp.cos(phase) * jnp.real(transformed) - jnp.sin(phase) * jnp.imag(transformed))
    return image * (1.0 / math.sqrt(VIS_ALL))
```

```python
import math

import jax
import jax.numpy as jnp
import numpy as np
from jax import lax
from jax.experimental import pallas as pl
from jax.experimental.pallas import tpu as pltpu
from jax.sharding import Mesh
from jax.sharding import PartitionSpec as P

G = 4096
TILE = ("tile_0", "tile_1", "tile_2")
PLANE = ("plane_0", "plane_1")
PLANE_TILE = PLANE + TILE
BANDS = 16
CAP = 32
PAIR = 2
COLS = 128
SETS = PAIR * BANDS
GROUPS = 32

SIN = (6.283183359351797, -41.341456456971535, 81.59688036372165, -76.58598132852413,
       41.227609837804344, -12.302204294679466)
COS = (0.9999996601928737, -19.739032170917408, 64.93001305163173, -85.28516993938109,
       58.84794870978477, -21.158227293307913)


def horner(u, coefs):
    total = jnp.full_like(u, coefs[-1])
    for c in coefs[-2::-1]:
        total = total * u + c
    return total


def cis(turn):
    u = turn * turn
    return horner(u, COS), turn * horner(u, SIN)


def cis_int(k):
    return cis((((k + 2048) & 4095) - 2048).astype(jnp.float32) * (1.0 / 4096))


def mul(a, b):
    return a[0] * b[0] - a[1] * b[1], a[0] * b[1] + a[1] * b[0]


def add(a, b):
    return a[0] + b[0], a[1] + b[1]


def sub(a, b):
    return a[0] - b[0], a[1] - b[1]


def turned(a, k, n):
    k = k % n
    if k == 0:
        return a
    if 4 * k == n:
        return -a[1], a[0]
    if 8 * k == n:
        h = math.sqrt(0.5)
        return (a[0] - a[1]) * h, (a[0] + a[1]) * h
    if 8 * k == 3 * n:
        h = math.sqrt(0.5)
        return (-a[0] - a[1]) * h, (a[0] - a[1]) * h
    c, s = math.cos(2 * math.pi * k / n), math.sin(2 * math.pi * k / n)
    return a[0] * c - a[1] * s, a[0] * s + a[1] * c


def fft(xs):
    n = len(xs)
    if n == 1:
        return xs
    even, odd = fft(xs[0::2]), fft(xs[1::2])
    odd = [turned(o, k, n) for k, o in enumerate(odd)]
    return [add(e, o) for e, o in zip(even, odd)] + [sub(e, o) for e, o in zip(even, odd)]


def dft_matrix():
    n = 256
    k = np.outer(np.arange(n), np.arange(n)) % n
    w = np.concatenate([np.cos(2 * np.pi * k / n), np.sin(2 * np.pi * k / n)]).astype(np.float32)
    hi = w.astype(jnp.bfloat16)
    lo = (w - hi.astype(np.float32)).astype(jnp.bfloat16)
    return np.concatenate([hi, lo, hi], axis=1)


def kernel(first_ref, w_ref, taps_ref, vis_ref, dft_ref, out_ref, p_ref, q_ref, o_ref, e_ref, h_ref, y_ref):
    first = first_ref[0]

    def set_step(s, carry):
        off = vis_ref[2, s].astype(jnp.int32)
        col = off & (G - 1)
        row = off >> 12
        place = ((row & 15) << 4) | (row >> 4)
        p_ref[16] = place.astype(jnp.float32)
        base = (vis_ref[0, s], vis_ref[1, s])
        one = cis_int(col)
        base = mul(base, cis_int(col * first))
        power = one
        q_ref[0] = jnp.ones((GROUPS, 128), jnp.float32)
        q_ref[16] = jnp.zeros((GROUPS, 128), jnp.float32)
        for k in range(1, 16):
            q_ref[k] = power[0]
            q_ref[16 + k] = power[1]
            power = mul(power, one)
        for k in range(8):
            p_ref[k] = base[0]
            p_ref[8 + k] = base[1]
            if k < 7:
                base = mul(base, power)

        rows = lax.broadcasted_iota(jnp.int32, (256, 128), 0).astype(jnp.float32)

        def group_step(g, c):
            lanes = pl.ds(pl.multiple_of(g * 128, 128), 128)
            here = p_ref[16, pl.ds(g, 1), :]
            o_ref[:, lanes] = jnp.where(rows == here, 1.0, 0.0).astype(jnp.bfloat16)
            qr = q_ref[0:16, pl.ds(g, 1), :].reshape(16, 128)
            qi = q_ref[16:32, pl.ds(g, 1), :].reshape(16, 128)
            for k in range(8):
                pr = p_ref[k, pl.ds(g, 1), :]
                pi = p_ref[8 + k, pl.ds(g, 1), :]
                e_ref[16 * k : 16 * k + 16, lanes] = (pr * qr - pi * qi).astype(jnp.bfloat16)
                e_ref[128 + 16 * k : 144 + 16 * k, lanes] = (pr * qi + pi * qr).astype(jnp.bfloat16)
            return c

        lax.fori_loop(0, GROUPS, group_step, 0)
        acc = lax.dot_general(
            o_ref[...], e_ref[...], (((1,), (1,)), ((), ())), preferred_element_type=jnp.float32
        )
        plane = s // BANDS
        at = pl.ds(pl.multiple_of((s % BANDS) * 16, 16), 16)
        for k in range(16):
            h_ref[plane * 16 + k, at, :] = acc[16 * k : 16 * k + 16, :]
        return carry

    lax.fori_loop(0, SETS, set_step, 0)

    def dft_step(k, carry):
        x = h_ref[k]
        hi = x.astype(jnp.bfloat16)
        lo = (x - hi.astype(jnp.float32)).astype(jnp.bfloat16)
        both = jnp.concatenate([hi, hi, lo], axis=0)
        r = jnp.dot(dft_ref[...], both, preferred_element_type=jnp.float32)
        y_ref[k, :, 0:128] = r[:256, :128] - r[256:, 128:]
        y_ref[k, :, 128:256] = r[:256, 128:] + r[256:, :128]
        return carry

    lax.fori_loop(0, PAIR * 16, dft_step, 0)

    lane = lax.broadcasted_iota(jnp.int32, (8, 128), 1) + first
    sub_row = lax.broadcasted_iota(jnp.int32, (8, 128), 0)
    step = cis_int(lane)
    weight = [taps_ref[k].astype(jnp.bfloat16).astype(jnp.float32) * (1.0 / 512) for k in range(8)]
    b = (jnp.full((8, 128), weight[7]), jnp.zeros((8, 128), jnp.float32))
    for k in range(6, -1, -1):
        b = mul(b, step)
        b = (b[0] + weight[k], b[1])

    def cosine(index):
        return (((index + 2048) & 4095) - 2048).astype(jnp.float32) * (0.5 / G)

    y2 = cosine(lane)
    y2 = y2 * y2

    def tile_step(t, carry):
        at = pl.ds(pl.multiple_of(t * 8, 8), 8)
        line = sub_row + t * 8
        tw = [None, cis_int(line)]
        for k in range(2, 16):
            tw.append(mul(tw[k // 2], tw[k - k // 2]))
        sums = None
        for q in range(PAIR):
            xs = []
            for k in range(16):
                x = (y_ref[q * 16 + k, at, 0:128], y_ref[q * 16 + k, at, 128:256])
                xs.append(x if k == 0 else mul(x, tw[k]))
            f = fft(xs)
            new = []
            for j in range(16):
                x2 = cosine(line + 256 * j)
                s = x2 * x2 + y2
                n = -s / (1.0 + jnp.sqrt(1.0 - s))
                turn = w_ref[q] * n
                turn = turn - jnp.round(turn)
                term = mul(f[j], cis(turn))
                new.append(term if sums is None else add(sums[j], term))
            sums = new
        zero = jnp.zeros((8, 128), jnp.float32)
        ts = [(jnp.full((8, 128), taps_ref[0]), zero)]
        ts += [(tw[k][0] * taps_ref[k], tw[k][1] * taps_ref[k]) for k in range(1, 8)]
        ts += [(zero, zero)] * 8
        a = fft(ts)
        for j in range(16):
            ab = mul(a[j], b)
            out_ref[pl.ds(pl.multiple_of(t * 8 + 256 * j, 8), 8), :] = sums[j][0] * ab[0] - sums[j][1] * ab[1]
        return carry

    lax.fori_loop(0, 32, tile_step, 0)


def part_image(first, w, taps, vis, interpret=False):
    smem = pl.BlockSpec(memory_space=pltpu.SMEM)
    vmem = pl.BlockSpec(memory_space=pltpu.VMEM)
    return pl.pallas_call(
        kernel,
        out_shape=jax.ShapeDtypeStruct((G, COLS), jnp.float32),
        in_specs=[smem, smem, smem, vmem, vmem],
        out_specs=vmem,
        scratch_shapes=[
            pltpu.VMEM((17, GROUPS, 128), jnp.float32),
            pltpu.VMEM((32, GROUPS, 128), jnp.float32),
            pltpu.VMEM((256, GROUPS * 128), jnp.bfloat16),
            pltpu.VMEM((256, GROUPS * 128), jnp.bfloat16),
            pltpu.VMEM((PAIR * 16, 256, 256), jnp.float32),
            pltpu.VMEM((PAIR * 16, 256, 256), jnp.float32),
        ],
        compiler_params=pltpu.CompilerParams(vmem_limit_bytes=56 * 1024 * 1024),
        interpret=interpret,
    )(first, w, taps, vis, dft_matrix())


def local(visibility, target, offset, taps, w_plane):
    dest = target[:, 0]
    onehot = (dest[:, None] == jnp.arange(128, dtype=jnp.int32)[None, :]).astype(jnp.int32)
    rank = jnp.sum(jnp.cumsum(onehot, axis=0) * onehot, axis=1) - 1
    plane, band = dest // BANDS, dest % BANDS
    bucket = ((plane % 4) * 2 + plane // 4) * BANDS + band
    slot = bucket * CAP + rank
    payload = jnp.stack([visibility[0], visibility[1], offset.astype(jnp.float32)])
    outgoing = jnp.zeros((3, 128 * CAP), jnp.float32).at[:, slot].set(payload)
    outgoing = outgoing.reshape(3, 4, SETS, CAP).transpose(1, 0, 2, 3).reshape(4, 3 * SETS, CAP)
    mine = lax.all_to_all(outgoing, "plane_1", split_axis=0, concat_axis=0, tiled=True)
    mine = mine.transpose(1, 0, 2).reshape(3 * SETS, 4 * CAP)
    mine = jnp.concatenate([mine, jnp.broadcast_to(w_plane[0], (8, 128))])
    everyone = lax.all_gather(mine, ("plane_0",) + TILE, axis=0)
    w = everyone[:, 3 * SETS, 0].reshape(2, 16)[:, 0]
    vis = everyone[:, : 3 * SETS].transpose(1, 0, 2).reshape(3, SETS, GROUPS, 128)
    first = lax.axis_index(TILE) * 256 + lax.axis_index("plane_0") * COLS
    part = part_image(first.reshape(1).astype(jnp.int32), w, taps, vis)
    arrived = lax.all_to_all(part, PLANE, split_axis=0, concat_axis=0, tiled=True)
    total = arrived.reshape(2, 4, 512, COLS).sum(axis=1)
    return jnp.concatenate([total[0], total[1]], axis=1)


def solution(mesh):
    finer = Mesh(
        mesh.devices.reshape(2, 4, 2, 4, 2), ("plane_0", "plane_1", "tile_0", "tile_1", "tile_2")
    )
    return jax.shard_map(
        local,
        mesh=finer,
        in_specs=(P(None, PLANE_TILE), P(PLANE_TILE, None), P(PLANE_TILE), P(), P(PLANE)),
        out_specs=P(PLANE, TILE),
        check_vma=False,
    )
```

```python
import math

import jax
import jax.numpy as jnp
import numpy as np
from jax import lax
from jax.experimental import pallas as pl
from jax.experimental.pallas import tpu as pltpu
from jax.sharding import Mesh
from jax.sharding import PartitionSpec as P

G = 4096
TILE = ("tile_0", "tile_1", "tile_2")
PLANE = ("plane_0", "plane_1")
PLANE_TILE = PLANE + TILE
BANDS = 16
CAP = 32
PAIR = 2
COLS = 128
SETS = PAIR * BANDS
UNROLL = 32
SKIP = 33
ROWS = 3 * 32 + 8
GROUPS = 32

SIN = (6.283183359351797, -41.341456456971535, 81.59688036372165, -76.58598132852413,
       41.227609837804344, -12.302204294679466)
COS = (0.9999996601928737, -19.739032170917408, 64.93001305163173, -85.28516993938109,
       58.84794870978477, -21.158227293307913)


def horner(u, coefs):
    total = jnp.full_like(u, coefs[-1])
    for c in coefs[-2::-1]:
        total = total * u + c
    return total


def cis(turn):
    u = turn * turn
    return horner(u, COS), turn * horner(u, SIN)


def cis_int(k):
    return cis((((k + 2048) & 4095) - 2048).astype(jnp.float32) * (1.0 / 4096))


def cis_half(k):
    return cis((((k + 4096) & 8191) - 4096).astype(jnp.float32) * (1.0 / 8192))


def mul(a, b):
    return a[0] * b[0] - a[1] * b[1], a[0] * b[1] + a[1] * b[0]


def add(a, b):
    return a[0] + b[0], a[1] + b[1]


def sub(a, b):
    return a[0] - b[0], a[1] - b[1]


def turned(a, k, n):
    k = k % n
    if k == 0:
        return a
    if 4 * k == n:
        return -a[1], a[0]
    if 8 * k == n:
        h = math.sqrt(0.5)
        return (a[0] - a[1]) * h, (a[0] + a[1]) * h
    if 8 * k == 3 * n:
        h = math.sqrt(0.5)
        return (-a[0] - a[1]) * h, (a[0] - a[1]) * h
    c, s = math.cos(2 * math.pi * k / n), math.sin(2 * math.pi * k / n)
    return a[0] * c - a[1] * s, a[0] * s + a[1] * c


def fft(xs):
    n = len(xs)
    if n == 1:
        return xs
    even, odd = fft(xs[0::2]), fft(xs[1::2])
    odd = [turned(o, k, n) for k, o in enumerate(odd)]
    return [add(e, o) for e, o in zip(even, odd)] + [sub(e, o) for e, o in zip(even, odd)]


def dft_matrix():
    n = 256
    k = np.outer(np.arange(n), np.arange(n)) % n
    w = np.concatenate([np.cos(2 * np.pi * k / n), np.sin(2 * np.pi * k / n)]).astype(np.float32)
    hi = w.astype(jnp.bfloat16)
    lo = (w - hi.astype(np.float32)).astype(jnp.bfloat16)
    return np.concatenate([hi, lo, hi], axis=1)


def kernel(
    first_ref, taps_ref, *refs
):
    vis_refs, refs = refs[:8], refs[8:]
    dft_ref, out_ref, p0_ref, p1_ref, q0_ref, q1_ref, acc_ref, h_ref, y_ref = refs

    def values(v, s):
        rows = pl.ds(pl.multiple_of(4 * (v * SETS + s), 4), 4)
        return jnp.concatenate([ref[rows, :] for ref in vis_refs])

    first = first_ref[0]

    def tables(s, p_ref, q_ref):
        off = values(2, s).astype(jnp.int32)
        col = off & (G - 1)
        row = off >> 12
        p_ref[pl.ds(16 * GROUPS, GROUPS), :] = (row & 15).astype(jnp.float32)
        p_ref[pl.ds(17 * GROUPS, GROUPS), :] = (row >> 4).astype(jnp.float32)
        half = cis_half(col)
        one = mul(half, half)
        base = mul((values(0, s), values(1, s)), cis_half(col * (2 * first + 15)))
        power = half
        for k in range(8):
            q_ref[pl.ds(k * SKIP, GROUPS), :] = power[0]
            q_ref[pl.ds((8 + k) * SKIP, GROUPS), :] = power[1]
            if k < 7:
                power = mul(power, one)
        step = one
        for k in range(4):
            step = mul(step, step)
        for k in range(8):
            p_ref[pl.ds(k * GROUPS, GROUPS), :] = base[0]
            p_ref[pl.ds((8 + k) * GROUPS, GROUPS), :] = base[1]
            if k < 7:
                base = mul(base, step)

    sub16 = lax.broadcasted_iota(jnp.int32, (16, 128), 0).astype(jnp.float32).astype(jnp.bfloat16)
    yes = jnp.ones((16, 128), jnp.bfloat16)
    no = jnp.zeros((16, 128), jnp.bfloat16)

    def made(g, p_ref, q_ref):
        def spread(row):
            return jnp.broadcast_to(p_ref[pl.ds(row * GROUPS + g, 1), :], (16, 128)).astype(jnp.bfloat16)

        high = jnp.where(spread(17) == sub16, spread(16), -yes)
        o = [jnp.where(high == jnp.bfloat16(k), yes, no) for k in range(16)]
        qr = q_ref[pl.ds(g, 8, stride=SKIP), :]
        qi = q_ref[pl.ds(8 * SKIP + g, 8, stride=SKIP), :]
        products = []
        for part, q in ((0, qr), (8, qi), (0, qi), (8, qr)):
            for k in range(0, 8, 2):
                two = [p_ref[pl.ds((part + k + j) * GROUPS + g, 1), :] * q for j in range(2)]
                products.append(jnp.concatenate(two).astype(jnp.bfloat16))
        return jnp.concatenate(o), jnp.concatenate(products)

    def phase(used, later, s):
        def chunk(k, c):
            parts = [made(k * UNROLL + j, *used) for j in range(UNROLL)]
            o = jnp.concatenate([x[0] for x in parts], axis=1)
            e = jnp.concatenate([x[1] for x in parts], axis=1)
            part = lax.dot_general(o, e, (((1,), (1,)), ((), ())), preferred_element_type=jnp.float32)
            if UNROLL == GROUPS:
                put(part)
            else:
                acc_ref[...] += part
            return c

        plane = s // BANDS
        at = pl.ds(pl.multiple_of((s % BANDS) * 16, 16), 16)

        def put(part):
            for k in range(16):
                h_ref[plane * 16 + k, at, :] = part[16 * k : 16 * k + 16, :]

        tables(jnp.minimum(s + 1, SETS - 1), *later)
        if UNROLL == GROUPS:
            chunk(0, 0)
        else:
            acc_ref[...] = jnp.zeros((256, 256), jnp.float32)
            lax.fori_loop(0, GROUPS // UNROLL, chunk, 0)
            put(acc_ref[...])

    buf0, buf1 = (p0_ref, q0_ref), (p1_ref, q1_ref)
    tables(0, *buf0)

    def two_sets(i, c):
        phase(buf0, buf1, 2 * i)
        phase(buf1, buf0, 2 * i + 1)
        return c

    lax.fori_loop(0, SETS // 2, two_sets, 0)

    sign = jnp.where(lax.broadcasted_iota(jnp.int32, (256, 128), 1) < 64, -1.0, 1.0)

    def dft_step(i, carry):
        for j in range(2):
            k = 2 * i + j
            re, im = h_ref[k, :, 0:128], h_ref[k, :, 128:256]
            re = re + sign * pltpu.roll(re, 64, 1)
            im = im - sign * pltpu.roll(im, 64, 1)
            x = jnp.concatenate([re, im], axis=1)
            hi = x.astype(jnp.bfloat16)
            lo = (x - hi.astype(jnp.float32)).astype(jnp.bfloat16)
            both = jnp.concatenate([hi, hi, lo], axis=0)
            r = jnp.dot(dft_ref[...], both, preferred_element_type=jnp.float32)
            y_ref[k, :, 0:128] = r[:256, :128] - r[256:, 128:]
            y_ref[k, :, 128:256] = r[:256, 128:] + r[256:, :128]
        return carry

    lax.fori_loop(0, PAIR * 8, dft_step, 0)

    place = lax.broadcasted_iota(jnp.int32, (8, 128), 1)
    lower = place & 63
    lane = 2 * (lower - (lower & 7)) + jnp.where(place < 64, 8 + (lower & 7), 7 - (lower & 7))
    inner = place & 15
    source = ((place - inner) >> 1) + jnp.where(inner < 8, 71 - inner, inner - 8)
    lane = lane + first
    sub_row = lax.broadcasted_iota(jnp.int32, (8, 128), 0)
    step = cis_int(lane)
    weight = [taps_ref[k].astype(jnp.bfloat16).astype(jnp.float32) * (1.0 / 512) for k in range(8)]
    b = (jnp.full((8, 128), weight[7]), jnp.zeros((8, 128), jnp.float32))
    for k in range(6, -1, -1):
        b = mul(b, step)
        b = (b[0] + weight[k], b[1])

    def cosine(index):
        return (((index + 2048) & 4095) - 2048).astype(jnp.float32) * (0.5 / G)

    y2 = cosine(lane)
    y2 = y2 * y2
    w_row = sum(ref[pl.ds(4 * 3 * SETS, 1), :] for ref in vis_refs[:4]) * 0.5
    w = [jnp.broadcast_to(w_row[:, q : q + 1], (8, 128)) for q in range(PAIR)]

    def tile_step(t, carry):
        at = pl.ds(pl.multiple_of(t * 8, 8), 8)
        line = sub_row + t * 8
        tw = [None, cis_int(line)]
        for k in range(2, 16):
            tw.append(mul(tw[k // 2], tw[k - k // 2]))
        sums = None
        for q in range(PAIR):
            xs = []
            for k in range(16):
                x = (y_ref[q * 16 + k, at, 0:128], y_ref[q * 16 + k, at, 128:256])
                xs.append(x if k == 0 else mul(x, tw[k]))
            f = fft(xs)
            new = []
            for j in range(16):
                x2 = cosine(line + 256 * j)
                s = x2 * x2 + y2
                n = -s / (1.0 + jnp.sqrt(1.0 - s))
                turn = w[q] * n
                turn = turn - jnp.round(turn)
                term = mul(f[j], cis(turn))
                new.append(term if sums is None else add(sums[j], term))
            sums = new
        zero = jnp.zeros((8, 128), jnp.float32)
        ts = [(jnp.full((8, 128), taps_ref[0]), zero)]
        ts += [(tw[k][0] * taps_ref[k], tw[k][1] * taps_ref[k]) for k in range(1, 8)]
        ts += [(zero, zero)] * 8
        a = fft(ts)
        for j in range(16):
            ab = mul(a[j], b)
            pixel = sums[j][0] * ab[0] - sums[j][1] * ab[1]
            rows = pl.ds(pl.multiple_of(t * 8 + 256 * j, 8), 8)
            out_ref[rows, :] = jnp.take_along_axis(pixel, source, axis=1)
        return carry

    lax.fori_loop(0, 32, tile_step, 0)


def part_image(first, taps, *vis, interpret=False):
    smem = pl.BlockSpec(memory_space=pltpu.SMEM)
    vmem = pl.BlockSpec(memory_space=pltpu.VMEM)
    return pl.pallas_call(
        kernel,
        out_shape=jax.ShapeDtypeStruct((G, COLS), jnp.float32),
        in_specs=[smem, smem] + [vmem] * 9,
        out_specs=vmem,
        scratch_shapes=[
            pltpu.VMEM((18 * GROUPS, 128), jnp.float32),
            pltpu.VMEM((18 * GROUPS, 128), jnp.float32),
            pltpu.VMEM((16 * SKIP, 128), jnp.float32),
            pltpu.VMEM((16 * SKIP, 128), jnp.float32),
            pltpu.VMEM((256, 256), jnp.float32),
            pltpu.VMEM((PAIR * 16, 256, 256), jnp.float32),
            pltpu.VMEM((PAIR * 16, 256, 256), jnp.float32),
        ],
        compiler_params=pltpu.CompilerParams(vmem_limit_bytes=56 * 1024 * 1024),
        interpret=interpret,
    )(first, taps, *vis, dft_matrix())


def shifted(x, axis, by):
    length = lax.axis_size(axis)
    return lax.ppermute(x, axis, [(i, (i + by) % length) for i in range(length)])


def local(visibility, target, offset, taps, w_plane):
    dest = target[:, 0]
    onehot = (dest[:, None] == jnp.arange(128, dtype=jnp.int32)[None, :]).astype(jnp.int32)
    rank = jnp.sum(jnp.cumsum(onehot, axis=0) * onehot, axis=1) - 1
    plane, band = dest // BANDS, dest % BANDS
    bucket = ((plane % 4) * 2 + plane // 4) * BANDS + band
    slot = bucket * CAP + rank
    payload = jnp.stack([visibility[0], visibility[1], offset.astype(jnp.float32)])
    outgoing = jnp.zeros((3, 128 * CAP), jnp.float32).at[:, slot].set(payload)
    outgoing = outgoing.reshape(3, 4, SETS, CAP).transpose(1, 0, 2, 3).reshape(4, 3 * SETS, CAP)
    here = lax.axis_index("plane_1")
    mine = []
    for by in range(4):
        block = lax.dynamic_index_in_dim(outgoing, (here + by) % 4, 0, keepdims=False)
        mine.append(block if by == 0 else shifted(block, "plane_1", by))
    mine = jnp.concatenate(mine, axis=1)
    half = lax.axis_index("plane_0")
    w_row = jnp.where(jnp.arange(128) == half, w_plane[0], 0.0)
    mine = jnp.concatenate([mine, jnp.broadcast_to(w_row, (8, 128))])
    line = [mine] + [shifted(mine, "tile_1", by) for by in (1, 2, 3)]
    line = jnp.stack(line, axis=1).reshape(ROWS * 4, 128)
    area = [line] + [shifted(line, ("plane_0", "tile_0"), by) for by in (1, 2, 3)]
    area = area + [shifted(x, "tile_2", 1) for x in area]
    first = lax.axis_index(TILE) * 256 + half * COLS
    part = part_image(first.reshape(1).astype(jnp.int32), taps, *area)
    arrived = lax.all_to_all(part, PLANE, split_axis=0, concat_axis=0, tiled=True)
    total = arrived.reshape(2, 4, 512, COLS).sum(axis=1)
    return jnp.concatenate([total[0], total[1]], axis=1)


def solution(mesh):
    finer = Mesh(
        mesh.devices.reshape(2, 4, 2, 4, 2), ("plane_0", "plane_1", "tile_0", "tile_1", "tile_2")
    )
    return jax.shard_map(
        local,
        mesh=finer,
        in_specs=(P(None, PLANE_TILE), P(PLANE_TILE, None), P(PLANE_TILE), P(), P(PLANE)),
        out_specs=P(PLANE, TILE),
        check_vma=False,
    )
```

```python
import math

import jax
import jax.numpy as jnp
import numpy as np
from jax import lax
from jax.experimental import pallas as pl
from jax.experimental.pallas import tpu as pltpu
from jax.sharding import Mesh
from jax.sharding import PartitionSpec as P

G = 4096
TILE = ("tile_0", "tile_1", "tile_2")
PLANE = ("plane_0", "plane_1")
PLANE_TILE = PLANE + TILE
BANDS = 16
CAP = 32
PAIR = 2
COLS = 128
SETS = PAIR * BANDS
SKIP = 33
DFTS = 4
ROWS = 3 * 32 + 8
GROUPS = 32

SIN = (6.283183359351797, -41.341456456971535, 81.59688036372165, -76.58598132852413,
       41.227609837804344, -12.302204294679466)
COS = (0.9999996601928737, -19.739032170917408, 64.93001305163173, -85.28516993938109,
       58.84794870978477, -21.158227293307913)


SIN4 = (6.283080178478066, -41.332270740282254, 81.3803723363611, -74.5450983459368, 32.89453310276785)
COS4 = (0.9999814280910587, -19.732589155128917, 64.69856260154607, -82.54685792407774, 45.912495330496334)


def horner(u, coefs):
    total = jnp.full_like(u, coefs[-1])
    for c in coefs[-2::-1]:
        total = total * u + c
    return total


def cis(turn):
    u = turn * turn
    return horner(u, COS), turn * horner(u, SIN)


def cis4(turn):
    u = turn * turn
    return horner(u, COS4), turn * horner(u, SIN4)


def cis_int(k):
    return cis((((k + 2048) & 4095) - 2048).astype(jnp.float32) * (1.0 / 4096))


def cis_half(k):
    return cis((((k + 4096) & 8191) - 4096).astype(jnp.float32) * (1.0 / 8192))


def mul(a, b):
    return a[0] * b[0] - a[1] * b[1], a[0] * b[1] + a[1] * b[0]


def add(a, b):
    if b is None:
        return a
    return a[0] + b[0], a[1] + b[1]


def sub(a, b):
    if b is None:
        return a
    return a[0] - b[0], a[1] - b[1]


def turned(a, k, n):
    k = k % n
    if a is None or k == 0:
        return a
    if 4 * k == n:
        return -a[1], a[0]
    if 8 * k == n:
        h = math.sqrt(0.5)
        return (a[0] - a[1]) * h, (a[0] + a[1]) * h
    if 8 * k == 3 * n:
        h = math.sqrt(0.5)
        return (-a[0] - a[1]) * h, (a[0] - a[1]) * h
    c, s = math.cos(2 * math.pi * k / n), math.sin(2 * math.pi * k / n)
    return a[0] * c - a[1] * s, a[0] * s + a[1] * c


def fft(xs):
    n = len(xs)
    if n == 1:
        return xs
    even, odd = fft(xs[0::2]), fft(xs[1::2])
    odd = [turned(o, k, n) for k, o in enumerate(odd)]
    return [add(e, o) for e, o in zip(even, odd)] + [sub(e, o) for e, o in zip(even, odd)]


def dft_matrix():
    n = 256
    k = np.outer(np.arange(n), np.arange(n)) % n
    w = np.concatenate([np.cos(2 * np.pi * k / n), np.sin(2 * np.pi * k / n)]).astype(np.float32)
    hi = w.astype(jnp.bfloat16)
    lo = (w - hi.astype(np.float32)).astype(jnp.bfloat16)
    return np.concatenate([hi, lo, hi], axis=1)


def bucket_kernel(here_ref, dest_ref, off_ref, vis_ref, *out_refs):
    dest = dest_ref[...]
    plane, band = dest >> 4, dest & 15
    spot = (((plane - here_ref[0]) & 3) * 2 + (plane >> 2)) * BANDS + band
    low, high = (spot & 15).astype(jnp.float32), (spot >> 4).astype(jnp.float32)
    off = off_ref[...]
    pieces = []
    for v in range(2):
        x = vis_ref[v]
        top = x.astype(jnp.bfloat16).astype(jnp.float32)
        pieces += [top, x - top]
    pieces += [(off >> 12).astype(jnp.float32), ((off >> 4) & 255).astype(jnp.float32), (off & 15).astype(jnp.float32)]
    sub16 = lax.broadcasted_iota(jnp.int32, (16, 128), 0).astype(jnp.float32).astype(jnp.bfloat16)
    yes, no = jnp.ones((16, 128), jnp.bfloat16), jnp.zeros((16, 128), jnp.bfloat16)
    first = lax.broadcasted_iota(jnp.int32, (256, 256), 0) <= lax.broadcasted_iota(jnp.int32, (256, 256), 1)
    upto = jnp.where(first, 1.0, 0.0).astype(jnp.bfloat16)
    upto = jnp.concatenate([upto, jnp.ones((256, 256), jnp.bfloat16)])

    def spread(x, i):
        return jnp.broadcast_to(x[i : i + 1], (16, 128)).astype(jnp.bfloat16)

    ones = []
    for i in range(16):
        code = jnp.where(spread(low, i) == sub16, spread(high, i), -yes)
        ones.append([jnp.where(code == jnp.bfloat16(k), yes, no) for k in range(8)])
    slots = lax.broadcasted_iota(jnp.int32, (32, 256), 0).astype(jnp.float32)
    before = jnp.zeros((128, 256), jnp.bfloat16)
    ranked = []
    for i in range(8):
        one = jnp.concatenate([jnp.concatenate(ones[2 * i]), jnp.concatenate(ones[2 * i + 1])], axis=1)
        count = jnp.dot(jnp.concatenate([one, before], axis=1), upto, preferred_element_type=jnp.float32)
        before = before + one
        rank = jnp.sum(count * one.astype(jnp.float32), axis=0, keepdims=True) - 1.0
        ranked.append(jnp.where(slots == rank, 1.0, 0.0).astype(jnp.bfloat16))
    ranked = jnp.concatenate(ranked, axis=1)
    held = []
    for x in pieces:
        held.append(
            jnp.concatenate([jnp.concatenate([o * spread(x, i) for o in ones[i]]) for i in range(16)], axis=1)
        )
    r = lax.dot_general(
        jnp.concatenate(held), ranked, (((1,), (1,)), ((), ())), preferred_element_type=jnp.float32
    )
    r = [r[128 * k : 128 * k + 128] for k in range(7)]
    both = (r[0] + r[1], r[2] + r[3], r[4] * 4096.0 + r[5] * 16.0 + r[6])
    for x in range(4):
        for v in range(3):
            out_refs[x][SETS * v : SETS * v + SETS, :] = both[v][SETS * x : SETS * x + SETS]


def buckets(here, dest, off, vis, interpret=False):
    smem = pl.BlockSpec(memory_space=pltpu.SMEM)
    vmem = pl.BlockSpec(memory_space=pltpu.VMEM)
    return pl.pallas_call(
        bucket_kernel,
        out_shape=[jax.ShapeDtypeStruct((3 * SETS, CAP), jnp.float32)] * 4,
        in_specs=[smem, vmem, vmem, vmem],
        out_specs=[vmem] * 4,
        interpret=interpret,
    )(here, dest, off, vis)


def first_kernel(first_ref, taps_ref, *refs):
    vis_refs, refs = refs[:8], refs[8:]
    dft_ref, out_ref, p0_ref, p1_ref, q0_ref, q1_ref, h_ref, y_ref = refs
    first = first_ref[0]

    def values(v, s):
        rows = pl.ds(pl.multiple_of(4 * (v * SETS + s), 4), 4)
        return jnp.concatenate([ref[rows, :] for ref in vis_refs])

    def tables(s, p_ref, q_ref):
        off = values(2, s).astype(jnp.int32)
        col = off & (G - 1)
        row = off >> 12
        p_ref[pl.ds(16 * GROUPS, GROUPS), :] = (row & 15).astype(jnp.float32)
        p_ref[pl.ds(17 * GROUPS, GROUPS), :] = (row >> 4).astype(jnp.float32)
        half = cis_half(col)
        one = mul(half, half)
        base = mul((values(0, s), values(1, s)), cis_half(col * (2 * first + 15)))
        power = half
        for k in range(8):
            q_ref[pl.ds(k * SKIP, GROUPS), :] = power[0]
            q_ref[pl.ds((8 + k) * SKIP, GROUPS), :] = power[1]
            if k < 7:
                power = mul(power, one)
        step = one
        for k in range(4):
            step = mul(step, step)
        for k in range(8):
            p_ref[pl.ds(k * GROUPS, GROUPS), :] = base[0]
            p_ref[pl.ds((8 + k) * GROUPS, GROUPS), :] = base[1]
            if k < 7:
                base = mul(base, step)

    sub16 = lax.broadcasted_iota(jnp.int32, (16, 128), 0).astype(jnp.float32).astype(jnp.bfloat16)
    yes = jnp.ones((16, 128), jnp.bfloat16)
    no = jnp.zeros((16, 128), jnp.bfloat16)

    def made(g, p_ref, q_ref):
        def spread(row):
            return jnp.broadcast_to(p_ref[pl.ds(row * GROUPS + g, 1), :], (16, 128)).astype(jnp.bfloat16)

        high = jnp.where(spread(17) == sub16, spread(16), -yes)
        o = [jnp.where(high == jnp.bfloat16(k), yes, no) for k in range(16)]
        qr = q_ref[pl.ds(g, 8, stride=SKIP), :]
        qi = q_ref[pl.ds(8 * SKIP + g, 8, stride=SKIP), :]
        products = []
        for part, q in ((0, qr), (8, qi), (0, qi), (8, qr)):
            for k in range(0, 8, 2):
                two = [p_ref[pl.ds((part + k + j) * GROUPS + g, 1), :] * q for j in range(2)]
                products.append(jnp.concatenate(two).astype(jnp.bfloat16))
        return jnp.concatenate(o), jnp.concatenate(products)

    def phase(used, later, s):
        tables(jnp.minimum(s + 1, SETS - 1), *later)
        parts = [made(g, *used) for g in range(GROUPS)]
        o = jnp.concatenate([x[0] for x in parts], axis=1)
        e = jnp.concatenate([x[1] for x in parts], axis=1)
        part = lax.dot_general(o, e, (((1,), (1,)), ((), ())), preferred_element_type=jnp.float32)
        plane = s // BANDS
        at = pl.ds(pl.multiple_of((s % BANDS) * 16, 16), 16)
        for k in range(16):
            h_ref[plane * 16 + k, at, :] = part[16 * k : 16 * k + 16, :]

    buf0, buf1 = (p0_ref, q0_ref), (p1_ref, q1_ref)
    tables(0, *buf0)

    def two_sets(i, c):
        phase(buf0, buf1, 2 * i)
        phase(buf1, buf0, 2 * i + 1)
        return c

    lax.fori_loop(0, SETS // 2, two_sets, 0)

    w_row = sum(ref[pl.ds(4 * 3 * SETS, 1), :] for ref in vis_refs[:4]) * 0.5
    rows_of_image(first, taps_ref, w_row, dft_ref, h_ref, out_ref, y_ref)


def rows_of_image(first, taps_ref, w_row, dft_ref, h_ref, out_ref, y_ref):
    sign = jnp.where(lax.broadcasted_iota(jnp.int32, (256, 128), 1) < 64, -1.0, 1.0)

    def dft_step(i, carry):
        for j in range(DFTS):
            k = DFTS * i + j
            re, im = h_ref[k, :, 0:128], h_ref[k, :, 128:256]
            re = re + sign * pltpu.roll(re, 64, 1)
            im = im - sign * pltpu.roll(im, 64, 1)
            x = jnp.concatenate([re, im], axis=1)
            hi = x.astype(jnp.bfloat16)
            lo = (x - hi.astype(jnp.float32)).astype(jnp.bfloat16)
            both = jnp.concatenate([hi, hi, lo], axis=0)
            r = jnp.dot(dft_ref[...], both, preferred_element_type=jnp.float32)
            y_ref[k, :, 0:128] = r[:256, :128] - r[256:, 128:]
            y_ref[k, :, 128:256] = r[:256, 128:] + r[256:, :128]
        return carry

    lax.fori_loop(0, PAIR * 16 // DFTS, dft_step, 0)

    place = lax.broadcasted_iota(jnp.int32, (8, 128), 1)
    lower = place & 63
    lane = 2 * (lower - (lower & 7)) + jnp.where(place < 64, 8 + (lower & 7), 7 - (lower & 7))
    inner = place & 15
    source = ((place - inner) >> 1) + jnp.where(inner < 8, 71 - inner, inner - 8)
    lane = lane + first
    sub_row = lax.broadcasted_iota(jnp.int32, (8, 128), 0)
    step = cis_int(lane)
    weight = [taps_ref[k].astype(jnp.bfloat16).astype(jnp.float32) * (1.0 / 512) for k in range(8)]
    b = (jnp.full((8, 128), weight[7]), jnp.zeros((8, 128), jnp.float32))
    for k in range(6, -1, -1):
        b = mul(b, step)
        b = (b[0] + weight[k], b[1])

    scale = 0.5 / G
    y = (((lane + 2048) & 4095) - 2048).astype(jnp.float32) * scale
    rest = 1.0 - y * y
    w = [jnp.broadcast_to(w_row[:, q : q + 1], (8, 128)) for q in range(PAIR)]

    def tile_step(t, carry):
        at = pl.ds(pl.multiple_of(t * 8, 8), 8)
        line = sub_row + t * 8
        tw = [None, cis_int(line)]
        for k in range(2, 16):
            tw.append(mul(tw[k // 2], tw[k - k // 2]))
        x0 = line.astype(jnp.float32) * scale
        sums = None
        for q in range(PAIR):
            xs = []
            for k in range(16):
                x = (y_ref[q * 16 + k, at, 0:128], y_ref[q * 16 + k, at, 128:256])
                xs.append(x if k == 0 else mul(x, tw[k]))
            f = fft(xs)
            new = []
            for j in range(16):
                x = x0 + (256 * j if j < 8 else 256 * j - G) * scale
                z = rest - x * x
                turn = w[q] * (z * lax.rsqrt(z)) - w[q]
                turn = turn - jnp.round(turn)
                term = mul(f[j], cis4(turn))
                new.append(term if sums is None else add(sums[j], term))
            sums = new
        zero = jnp.zeros((8, 128), jnp.float32)
        ts = [(jnp.full((8, 128), taps_ref[0]), zero)]
        ts += [(tw[k][0] * taps_ref[k], tw[k][1] * taps_ref[k]) for k in range(1, 8)]
        ts += [None] * 8
        a = fft(ts)
        for j in range(16):
            ab = mul(a[j], b)
            pixel = sums[j][0] * ab[0] - sums[j][1] * ab[1]
            out_ref[j, at, :] = jnp.take_along_axis(pixel, source, axis=1)
        return carry

    lax.fori_loop(0, 256 // 8, tile_step, 0)


def part_image(first, taps, *vis, interpret=False):
    smem = pl.BlockSpec(memory_space=pltpu.SMEM)
    vmem = pl.BlockSpec(memory_space=pltpu.VMEM)
    return pl.pallas_call(
        first_kernel,
        out_shape=jax.ShapeDtypeStruct((16, 256, COLS), jnp.float32),
        in_specs=[smem, smem] + [vmem] * 9,
        out_specs=vmem,
        scratch_shapes=[
            pltpu.VMEM((18 * GROUPS, 128), jnp.float32),
            pltpu.VMEM((18 * GROUPS, 128), jnp.float32),
            pltpu.VMEM((16 * SKIP, 128), jnp.float32),
            pltpu.VMEM((16 * SKIP, 128), jnp.float32),
            pltpu.VMEM((PAIR * 16, 256, 256), jnp.float32),
            pltpu.VMEM((PAIR * 16, 256, 256), jnp.float32),
        ],
        compiler_params=pltpu.CompilerParams(vmem_limit_bytes=56 * 1024 * 1024),
        interpret=interpret,
    )(first, taps, *vis, dft_matrix())


def shifted(x, axis, by):
    length = lax.axis_size(axis)
    return lax.ppermute(x, axis, [(i, (i + by) % length) for i in range(length)])


def local(visibility, target, offset, taps, w_plane):
    here = lax.axis_index("plane_1").reshape(1).astype(jnp.int32)
    blocks = buckets(here, target.reshape(16, 128), offset.reshape(16, 128), visibility.reshape(2, 16, 128))
    mine = [blocks[0]] + [shifted(blocks[by], "plane_1", by) for by in (1, 2, 3)]
    mine = jnp.concatenate(mine, axis=1)
    half = lax.axis_index("plane_0")
    w_row = jnp.where(jnp.arange(128) == half, w_plane[0], 0.0)
    mine = jnp.concatenate([mine, jnp.broadcast_to(w_row, (8, 128))])
    line = [mine] + [shifted(mine, "tile_1", by) for by in (1, 2, 3)]
    line = jnp.stack(line, axis=1).reshape(ROWS * 4, 128)
    area = [line] + [shifted(line, ("plane_0", "tile_0"), by) for by in (1, 2, 3)]
    area = area + [shifted(x, "tile_2", 1) for x in area]
    first = lax.axis_index(TILE) * 256 + half * COLS
    first = first.reshape(1).astype(jnp.int32)
    part = part_image(first, taps, *area).reshape(G, COLS)
    arrived = lax.all_to_all(part, PLANE, split_axis=0, concat_axis=0, tiled=True)
    total = arrived.reshape(2, 4, 512, COLS).sum(axis=1)
    return jnp.concatenate([total[0], total[1]], axis=1)


def solution(mesh):
    finer = Mesh(
        mesh.devices.reshape(2, 4, 2, 4, 2), ("plane_0", "plane_1", "tile_0", "tile_1", "tile_2")
    )
    return jax.shard_map(
        local,
        mesh=finer,
        in_specs=(P(None, PLANE_TILE), P(PLANE_TILE, None), P(PLANE_TILE), P(), P(PLANE)),
        out_specs=P(PLANE, TILE),
        check_vma=False,
    )
```

```python
import math

import jax
import jax.numpy as jnp
import numpy as np
from jax import lax
from jax.experimental import pallas as pl
from jax.experimental.pallas import tpu as pltpu
from jax.sharding import Mesh
from jax.sharding import PartitionSpec as P

G = 4096
TILE = ("tile_0", "tile_1", "tile_2")
PLANE = ("plane_0", "plane_1")
PLANE_TILE = PLANE + TILE
BANDS = 16
CAP = 32
PAIR = 2
COLS = 128
SETS = PAIR * BANDS
SKIP = 33
STEPS = 2
GROUPS = 32

SIN = (6.283183359351797, -41.341456456971535, 81.59688036372165, -76.58598132852413,
       41.227609837804344, -12.302204294679466)
COS = (0.9999996601928737, -19.739032170917408, 64.93001305163173, -85.28516993938109,
       58.84794870978477, -21.158227293307913)


SIN4 = (6.283080178478066, -41.332270740282254, 81.3803723363611, -74.5450983459368, 32.89453310276785)
COS4 = (0.9999814280910587, -19.732589155128917, 64.69856260154607, -82.54685792407774, 45.912495330496334)


def horner(u, coefs):
    total = jnp.full_like(u, coefs[-1])
    for c in coefs[-2::-1]:
        total = total * u + c
    return total


def cis(turn):
    u = turn * turn
    return horner(u, COS), turn * horner(u, SIN)


def cis4(turn):
    u = turn * turn
    return horner(u, COS4), turn * horner(u, SIN4)


def cis_int(k):
    return cis((((k + 2048) & 4095) - 2048).astype(jnp.float32) * (1.0 / 4096))


def cis_half(k):
    return cis((((k + 4096) & 8191) - 4096).astype(jnp.float32) * (1.0 / 8192))


def mul(a, b):
    return a[0] * b[0] - a[1] * b[1], a[0] * b[1] + a[1] * b[0]


def add(a, b):
    if b is None:
        return a
    return a[0] + b[0], a[1] + b[1]


def sub(a, b):
    if b is None:
        return a
    return a[0] - b[0], a[1] - b[1]


def turned(a, k, n):
    k = k % n
    if a is None or k == 0:
        return a
    if 4 * k == n:
        return -a[1], a[0]
    if 8 * k == n:
        h = math.sqrt(0.5)
        return (a[0] - a[1]) * h, (a[0] + a[1]) * h
    if 8 * k == 3 * n:
        h = math.sqrt(0.5)
        return (-a[0] - a[1]) * h, (a[0] - a[1]) * h
    c, s = math.cos(2 * math.pi * k / n), math.sin(2 * math.pi * k / n)
    return a[0] * c - a[1] * s, a[0] * s + a[1] * c


def fft(xs):
    n = len(xs)
    if n == 1:
        return xs
    even, odd = fft(xs[0::2]), fft(xs[1::2])
    odd = [turned(o, k, n) for k, o in enumerate(odd)]
    return [add(e, o) for e, o in zip(even, odd)] + [sub(e, o) for e, o in zip(even, odd)]


def bucket_kernel(dest_ref, off_ref, vis_ref, out_ref):
    dest = jnp.concatenate([dest_ref[0:1, 128 * i : 128 * i + 128] for i in range(16)])
    plane, band = dest >> 4, dest & 15
    spot = ((plane & 3) * 2 + (plane >> 2)) * BANDS + band
    low, high = (spot & 15).astype(jnp.float32), (spot >> 4).astype(jnp.float32)
    off = off_ref[...]
    pieces = []
    for v in range(2):
        x = jnp.concatenate([vis_ref[v : v + 1, 128 * i : 128 * i + 128] for i in range(16)])
        top = x.astype(jnp.bfloat16).astype(jnp.float32)
        pieces += [top, x - top]
    pieces += [(off >> 12).astype(jnp.float32), ((off >> 4) & 255).astype(jnp.float32), (off & 15).astype(jnp.float32)]
    sub16 = lax.broadcasted_iota(jnp.int32, (16, 128), 0).astype(jnp.float32).astype(jnp.bfloat16)
    yes, no = jnp.ones((16, 128), jnp.bfloat16), jnp.zeros((16, 128), jnp.bfloat16)
    first = lax.broadcasted_iota(jnp.int32, (256, 256), 0) <= lax.broadcasted_iota(jnp.int32, (256, 256), 1)
    upto = jnp.where(first, 1.0, 0.0).astype(jnp.bfloat16)
    upto = jnp.concatenate([upto, jnp.ones((256, 256), jnp.bfloat16)])

    def spread(x, i):
        return jnp.broadcast_to(x[i : i + 1], (16, 128)).astype(jnp.bfloat16)

    ones = []
    for i in range(16):
        code = jnp.where(spread(low, i) == sub16, spread(high, i), -yes)
        ones.append([jnp.where(code == jnp.bfloat16(k), yes, no) for k in range(8)])
    quarter = ((spot & 3) * CAP).astype(jnp.float32)
    places = lax.broadcasted_iota(jnp.int32, (128, 256), 0).astype(jnp.float32)
    before = jnp.zeros((128, 256), jnp.bfloat16)
    placed = []
    for i in range(8):
        one = jnp.concatenate([jnp.concatenate(ones[2 * i]), jnp.concatenate(ones[2 * i + 1])], axis=1)
        count = jnp.dot(jnp.concatenate([one, before], axis=1), upto, preferred_element_type=jnp.float32)
        before = before + one
        rank = jnp.sum(count * one.astype(jnp.float32), axis=0, keepdims=True) - 1.0
        rank = rank + jnp.concatenate([quarter[2 * i : 2 * i + 1], quarter[2 * i + 1 : 2 * i + 2]], axis=1)
        placed.append(jnp.where(places == rank, 1.0, 0.0).astype(jnp.bfloat16))
    placed = jnp.concatenate(placed, axis=1)
    fours = (spot >> 2).astype(jnp.float32)
    rows = [[jnp.where(spread(fours, i) == sub16 + jnp.bfloat16(16 * k), yes, no) for k in range(2)] for i in range(16)]
    held = []
    for x in pieces:
        held.append(jnp.concatenate([jnp.concatenate([o * spread(x, i) for o in rows[i]]) for i in range(16)], axis=1))
    r = lax.dot_general(
        jnp.concatenate(held), placed, (((1,), (1,)), ((), ())), preferred_element_type=jnp.float32
    )
    r = [r[32 * k : 32 * k + 32] for k in range(7)]
    both = (r[0] + r[1], r[2] + r[3], r[4] * 4096.0 + r[5] * 16.0 + r[6])
    for i in range(16):
        x = i // 4
        for v in range(3):
            out_ref[i, 8 * v : 8 * v + 8, :] = both[v][8 * x : 8 * x + 8]


def buckets(dest, off, vis, interpret=False):
    vmem = pl.BlockSpec(memory_space=pltpu.VMEM)
    return pl.pallas_call(
        bucket_kernel,
        out_shape=jax.ShapeDtypeStruct((16, 24, 128), jnp.float32),
        in_specs=[vmem, vmem, vmem],
        out_specs=vmem,
        interpret=interpret,
    )(dest, off, vis)


def image_kernel(first_ref, *refs):
    own_refs, other_refs, refs = refs[:4], refs[4:8], refs[8:]
    out_ref, p0_ref, p1_ref, q0_ref, q1_ref, h0_ref, h1_ref, y0_ref, y1_ref, sum_ref, dft_ref, vis_ref = refs
    first = first_ref[0]
    segment = lax.broadcasted_iota(jnp.int32, (16, 128), 1) >> 5
    odd, upper = (segment & 1) == 1, segment >= 2

    def swapped(a, b, mask, by):
        return jnp.where(mask, pltpu.roll(b, by, 1), a), jnp.where(mask, b, pltpu.roll(a, 128 - by, 1))

    def regroup(step, c):
        for i in [step * 6 + k for k in range(6)]:
            for half, area in enumerate((own_refs, other_refs)):
                x = [ref[pl.ds(i, 16, stride=24), :] for ref in area]
                x[0], x[1] = swapped(x[0], x[1], odd, 32)
                x[2], x[3] = swapped(x[2], x[3], odd, 32)
                x[0], x[2] = swapped(x[0], x[2], upper, 64)
                x[1], x[3] = swapped(x[1], x[3], upper, 64)
                for j in range(4):
                    vis_ref[pl.ds(pl.multiple_of((4 * i + j) * GROUPS + 16 * half, 16), 16), :] = x[j]
        return c

    lax.fori_loop(0, 4, regroup, 0)

    def values(v, s):
        return vis_ref[pl.ds(pl.multiple_of((v * SETS + s) * GROUPS, GROUPS), GROUPS), :]

    def make_dft(i):
        k = 2 * (lax.broadcasted_iota(jnp.int32, (16, 256), 0) + 16 * i) + 1
        k = k * lax.broadcasted_iota(jnp.int32, (16, 256), 1) * 16
        for j, x in enumerate(cis_half(k)):
            rows = pl.ds(pl.multiple_of(128 * j + 16 * i, 16), 16)
            hi = x.astype(jnp.bfloat16)
            dft_ref[rows, 0:256] = hi
            dft_ref[rows, 256:512] = (x - hi.astype(jnp.float32)).astype(jnp.bfloat16)
            dft_ref[rows, 512:768] = hi

    def tables(s, p_ref, q_ref):
        off = values(2, s).astype(jnp.int32)
        col = off & (G - 1)
        row = off >> 12
        p_ref[pl.ds(16 * GROUPS, GROUPS), :] = (row & 15).astype(jnp.float32)
        p_ref[pl.ds(17 * GROUPS, GROUPS), :] = (row >> 4).astype(jnp.float32)
        half = cis_half(col)
        one = mul(half, half)
        base = mul((values(0, s), values(1, s)), cis_half(col * (2 * first + 15) - 16 * (row >> 4) - 256 * (s % BANDS)))
        power = half
        for k in range(8):
            q_ref[pl.ds(k * SKIP, GROUPS), :] = power[0]
            q_ref[pl.ds((8 + k) * SKIP, GROUPS), :] = power[1]
            if k < 7:
                power = mul(power, one)
        step = one
        for k in range(4):
            step = mul(step, step)
        for k in range(8):
            p_ref[pl.ds(k * GROUPS, GROUPS), :] = base[0]
            p_ref[pl.ds((8 + k) * GROUPS, GROUPS), :] = base[1]
            if k < 7:
                base = mul(base, step)

    sub16 = lax.broadcasted_iota(jnp.int32, (16, 128), 0).astype(jnp.float32).astype(jnp.bfloat16)
    yes = jnp.ones((16, 128), jnp.bfloat16)
    no = jnp.zeros((16, 128), jnp.bfloat16)

    def made(g, p_ref, q_ref):
        def spread(row):
            return jnp.broadcast_to(p_ref[pl.ds(row * GROUPS + g, 1), :], (16, 128)).astype(jnp.bfloat16)

        high = jnp.where(spread(17) == sub16, spread(16), -yes)
        o = [jnp.where(high == jnp.bfloat16(k), yes, no) for k in range(16)]
        qr = q_ref[pl.ds(g, 8, stride=SKIP), :]
        qi = q_ref[pl.ds(8 * SKIP + g, 8, stride=SKIP), :]
        products = []
        for part, q in ((0, qr), (8, qi), (0, qi), (8, qr)):
            for k in range(0, 8, 2):
                two = [p_ref[pl.ds((part + k + j) * GROUPS + g, 1), :] * q for j in range(2)]
                products.append(jnp.concatenate(two).astype(jnp.bfloat16))
        return jnp.concatenate(o), jnp.concatenate(products)

    def phase(used, later, s, h_ref):
        tables(jnp.minimum(s + 1, SETS - 1), *later)
        parts = [made(g, *used) for g in range(GROUPS)]
        o = jnp.concatenate([x[0] for x in parts], axis=1)
        e = jnp.concatenate([x[1] for x in parts], axis=1)
        part = lax.dot_general(o, e, (((1,), (1,)), ((), ())), preferred_element_type=jnp.float32)
        at = pl.ds(pl.multiple_of((s % BANDS) * 16, 16), 16)
        for k in range(16):
            h_ref[k, at, :] = part[16 * k : 16 * k + 16, :]

    sign = jnp.where(lax.broadcasted_iota(jnp.int32, (256, 128), 1) < 64, -1.0, 1.0)

    def dft(k, h_ref, y_ref):
        re, im = h_ref[k, :, 0:128], h_ref[k, :, 128:256]
        re = re + sign * pltpu.roll(re, 64, 1)
        im = im - sign * pltpu.roll(im, 64, 1)
        x = jnp.concatenate([re, im], axis=1)
        hi = x.astype(jnp.bfloat16)
        lo = (x - hi.astype(jnp.float32)).astype(jnp.bfloat16)
        both = jnp.concatenate([hi, hi, lo], axis=0)
        r = jnp.dot(dft_ref[...], both, preferred_element_type=jnp.float32)
        c_re, c_im, s_re, s_im = r[:128, :128], r[:128, 128:], r[128:, :128], r[128:, 128:]
        y_ref[k, 0:128, 0:128] = c_re - s_im
        y_ref[k, 0:128, 128:256] = c_im + s_re
        y_ref[k, 128:256, 0:128] = c_re + s_im
        y_ref[k, 128:256, 128:256] = c_im - s_re

    place = lax.broadcasted_iota(jnp.int32, (8, 128), 1)
    lower = place & 63
    lane = 2 * (lower - (lower & 7)) + jnp.where(place < 64, 8 + (lower & 7), 7 - (lower & 7))
    inner = place & 15
    source = ((place - inner) >> 1) + jnp.where(inner < 8, 71 - inner, inner - 8)
    lane = lane + first
    sub_row = lax.broadcasted_iota(jnp.int32, (8, 128), 0)
    scale = 0.5 / G
    y = (((lane + 2048) & 4095) - 2048).astype(jnp.float32) * scale
    rest = 1.0 - y * y
    def spread8(row, k):
        return jnp.broadcast_to(row[:, k : k + 1], (8, 128))

    w_row = sum(ref[384:385, :] for ref in own_refs) * 0.5
    taps_row = own_refs[0][385:386, :]

    def twiddles(line):
        tw = [None, cis_int(line)]
        for k in range(2, 16):
            tw.append(mul(tw[k // 2], tw[k - k // 2]))
        return tw

    def half_tile(t, half):
        line = sub_row + t * 8
        return pl.ds(pl.multiple_of(t * 8 + 128 * half, 8), 8), 255 - line if half else line

    def terms(at, line, tw, w, y_ref):
        xs = []
        for k in range(16):
            x = (y_ref[k, at, 0:128], y_ref[k, at, 128:256])
            xs.append(x if k == 0 else mul(x, tw[k]))
        f = fft(xs)
        x0 = line.astype(jnp.float32) * scale
        result = []
        for j in range(16):
            x = x0 + (256 * j if j < 8 else 256 * j - G) * scale
            z = rest - x * x
            turn = w * (z * lax.rsqrt(z)) - w
            turn = turn - jnp.round(turn)
            result.append(mul(f[j], cis4(turn)))
        return result

    buf0, buf1 = (p0_ref, q0_ref), (p1_ref, q1_ref)
    tables(0, *buf0)

    def sets_of_first(i, c):
        phase(buf0, buf1, 2 * i, h0_ref)
        phase(buf1, buf0, 2 * i + 1, h0_ref)
        make_dft(i)
        return c

    lax.fori_loop(0, BANDS // 2, sets_of_first, 0)

    def sets_of_second(i, c):
        phase(buf0, buf1, BANDS + 2 * i, h1_ref)
        dft(2 * i, h0_ref, y0_ref)
        phase(buf1, buf0, BANDS + 2 * i + 1, h1_ref)
        dft(2 * i + 1, h0_ref, y0_ref)
        return c

    lax.fori_loop(0, BANDS // 2, sets_of_second, 0)
    w0 = spread8(w_row, 0)

    def tiles_of_first(i, c):
        for k in range(STEPS):
            dft(STEPS * i + k, h1_ref, y1_ref)
        for k in range(STEPS):
            for half in range(2):
                at, line = half_tile(STEPS * i + k, half)
                for j, x in enumerate(terms(at, line, twiddles(line), w0, y0_ref)):
                    sum_ref[j, at, 0:128] = x[0]
                    sum_ref[j, at, 128:256] = x[1]
        return c

    lax.fori_loop(0, 16 // STEPS, tiles_of_first, 0)
    w1 = spread8(w_row, 1)
    taps = [spread8(taps_row, k) for k in range(8)]
    step = cis_int(lane)
    weight = [x.astype(jnp.bfloat16).astype(jnp.float32) * (1.0 / 512) for x in taps]
    b = (weight[7], jnp.zeros((8, 128), jnp.float32))
    for k in range(6, -1, -1):
        b = mul(b, step)
        b = (b[0] + weight[k], b[1])

    def tiles_of_second(t, c):
        for half in range(2):
            at, line = half_tile(t, half)
            tw = twiddles(line)
            ts = [(taps[0], jnp.zeros((8, 128), jnp.float32))]
            ts += [(tw[k][0] * taps[k], tw[k][1] * taps[k]) for k in range(1, 8)]
            a = fft(ts + [None] * 8)
            place = pl.ds(pl.multiple_of(248 - t * 8 if half else t * 8, 8), 8)
            for j, x in enumerate(terms(at, line, tw, w1, y1_ref)):
                x = add(x, (sum_ref[j, at, 0:128], sum_ref[j, at, 128:256]))
                ab = mul(a[j], b)
                pixel = jnp.take_along_axis(x[0] * ab[0] - x[1] * ab[1], source, axis=1)
                if half:
                    pixel = jnp.take_along_axis(pixel, 7 - sub_row, axis=0)
                out_ref[j, place, :] = pixel
        return c

    lax.fori_loop(0, 16, tiles_of_second, 0)


def part_image(first, *area, interpret=False):
    smem = pl.BlockSpec(memory_space=pltpu.SMEM)
    vmem = pl.BlockSpec(memory_space=pltpu.VMEM)
    return pl.pallas_call(
        image_kernel,
        out_shape=jax.ShapeDtypeStruct((16, 256, COLS), jnp.float32),
        in_specs=[smem] + [vmem] * 8,
        out_specs=vmem,
        scratch_shapes=[
            pltpu.VMEM((18 * GROUPS, 128), jnp.float32),
            pltpu.VMEM((18 * GROUPS, 128), jnp.float32),
            pltpu.VMEM((16 * SKIP, 128), jnp.float32),
            pltpu.VMEM((16 * SKIP, 128), jnp.float32),
            pltpu.VMEM((16, 256, 256), jnp.float32),
            pltpu.VMEM((16, 256, 256), jnp.float32),
            pltpu.VMEM((16, 256, 256), jnp.float32),
            pltpu.VMEM((16, 256, 256), jnp.float32),
            pltpu.VMEM((16, 256, 256), jnp.float32),
            pltpu.VMEM((256, 768), jnp.bfloat16),
            pltpu.VMEM((3 * SETS * GROUPS, 128), jnp.float32),
        ],
        compiler_params=pltpu.CompilerParams(vmem_limit_bytes=56 * 1024 * 1024),
        interpret=interpret,
    )(first, *area)


def shifted(x, axis, by):
    length = lax.axis_size(axis)
    return lax.ppermute(x, axis, [(i, (i + by) % length) for i in range(length)])


def local(visibility, target, offset, taps, w_plane):
    half = lax.axis_index("plane_0")
    out = buckets(target.reshape(1, 2048), offset.reshape(16, 128), visibility)
    own = lax.all_to_all(out, ("plane_1", "tile_1"), split_axis=0, concat_axis=0, tiled=True).reshape(384, 128)
    w_row = jnp.where(jnp.arange(128) == half, w_plane[0], 0.0)
    own = jnp.concatenate([own, w_row[None], jnp.pad(taps, (0, 120))[None], jnp.zeros((6, 128), jnp.float32)])
    area = [own] + [shifted(own, ("plane_0", "tile_0"), by) for by in (1, 2, 3)]
    area = area + [shifted(x, "tile_2", 1) for x in area]
    first = lax.axis_index(TILE) * 256 + half * COLS
    first = first.reshape(1).astype(jnp.int32)
    part = part_image(first, *area).reshape(G, COLS)
    arrived = lax.all_to_all(part, PLANE, split_axis=0, concat_axis=0, tiled=True)
    total = arrived.reshape(2, 4, 512, COLS).sum(axis=1)
    return jnp.concatenate([total[0], total[1]], axis=1)


def solution(mesh):
    finer = Mesh(
        mesh.devices.reshape(2, 4, 2, 4, 2), ("plane_0", "plane_1", "tile_0", "tile_1", "tile_2")
    )
    return jax.shard_map(
        local,
        mesh=finer,
        in_specs=(P(None, PLANE_TILE), P(PLANE_TILE, None), P(PLANE_TILE), P(), P(PLANE)),
        out_specs=P(PLANE, TILE),
        check_vma=False,
    )
```

```python
import math

import jax
import jax.numpy as jnp
import numpy as np
from jax import lax
from jax.experimental import pallas as pl
from jax.experimental.pallas import tpu as pltpu
from jax.sharding import Mesh
from jax.sharding import PartitionSpec as P

G = 4096
TILE = ("tile_0", "tile_1", "tile_2")
PLANE = ("plane_0", "plane_1")
PLANE_TILE = PLANE + TILE
BANDS = 16
CAP = 32
PAIR = 2
COLS = 128
SETS = PAIR * BANDS
SKIP = 33
STEPS = 2
GROUPS = 32

SIN = (6.283183359351797, -41.341456456971535, 81.59688036372165, -76.58598132852413,
       41.227609837804344, -12.302204294679466)
COS = (0.9999996601928737, -19.739032170917408, 64.93001305163173, -85.28516993938109,
       58.84794870978477, -21.158227293307913)


SIN4 = (6.283080178478066, -41.332270740282254, 81.3803723363611, -74.5450983459368, 32.89453310276785)
COS4 = (0.9999814280910587, -19.732589155128917, 64.69856260154607, -82.54685792407774, 45.912495330496334)


def horner(u, coefs):
    total = jnp.full_like(u, coefs[-1])
    for c in coefs[-2::-1]:
        total = total * u + c
    return total


def cis(turn):
    u = turn * turn
    return horner(u, COS), turn * horner(u, SIN)


def cis4(turn):
    u = turn * turn
    return horner(u, COS4), turn * horner(u, SIN4)


def cis_int(k):
    return cis((((k + 2048) & 4095) - 2048).astype(jnp.float32) * (1.0 / 4096))


def cis_half(k):
    return cis((((k + 4096) & 8191) - 4096).astype(jnp.float32) * (1.0 / 8192))


def mul(a, b):
    return a[0] * b[0] - a[1] * b[1], a[0] * b[1] + a[1] * b[0]


def add(a, b):
    if b is None:
        return a
    return a[0] + b[0], a[1] + b[1]


def sub(a, b):
    if b is None:
        return a
    return a[0] - b[0], a[1] - b[1]


def turned(a, k, n):
    k = k % n
    if a is None or k == 0:
        return a
    if 4 * k == n:
        return -a[1], a[0]
    if 8 * k == n:
        h = math.sqrt(0.5)
        return (a[0] - a[1]) * h, (a[0] + a[1]) * h
    if 8 * k == 3 * n:
        h = math.sqrt(0.5)
        return (-a[0] - a[1]) * h, (a[0] - a[1]) * h
    c, s = math.cos(2 * math.pi * k / n), math.sin(2 * math.pi * k / n)
    return a[0] * c - a[1] * s, a[0] * s + a[1] * c


def fft(xs):
    n = len(xs)
    if n == 1:
        return xs
    even, odd = fft(xs[0::2]), fft(xs[1::2])
    odd = [turned(o, k, n) for k, o in enumerate(odd)]
    return [add(e, o) for e, o in zip(even, odd)] + [sub(e, o) for e, o in zip(even, odd)]


def bucket_kernel(dest_ref, off_ref, vis_ref, out_ref):
    dest = jnp.concatenate([dest_ref[0:1, 128 * i : 128 * i + 128] for i in range(16)])
    plane, band = dest >> 4, dest & 15
    spot = ((plane & 3) * 2 + (plane >> 2)) * BANDS + band
    low, high = (spot & 15).astype(jnp.float32), (spot >> 4).astype(jnp.float32)
    off = off_ref[...]
    pieces = []
    for v in range(2):
        x = jnp.concatenate([vis_ref[v : v + 1, 128 * i : 128 * i + 128] for i in range(16)])
        top = x.astype(jnp.bfloat16).astype(jnp.float32)
        pieces += [top, x - top]
    pieces += [(off >> 12).astype(jnp.float32), ((off >> 4) & 255).astype(jnp.float32), (off & 15).astype(jnp.float32)]
    sub16 = lax.broadcasted_iota(jnp.int32, (16, 128), 0).astype(jnp.float32).astype(jnp.bfloat16)
    yes, no = jnp.ones((16, 128), jnp.bfloat16), jnp.zeros((16, 128), jnp.bfloat16)
    first = lax.broadcasted_iota(jnp.int32, (256, 256), 0) <= lax.broadcasted_iota(jnp.int32, (256, 256), 1)
    upto = jnp.where(first, 1.0, 0.0).astype(jnp.bfloat16)
    upto = jnp.concatenate([upto, jnp.ones((256, 256), jnp.bfloat16)])

    def spread(x, i):
        return jnp.broadcast_to(x[i : i + 1], (16, 128)).astype(jnp.bfloat16)

    ones = []
    for i in range(16):
        code = jnp.where(spread(low, i) == sub16, spread(high, i), -yes)
        ones.append([jnp.where(code == jnp.bfloat16(k), yes, no) for k in range(8)])
    quarter = ((spot & 3) * CAP).astype(jnp.float32)
    places = lax.broadcasted_iota(jnp.int32, (128, 256), 0).astype(jnp.float32)
    before = jnp.zeros((128, 256), jnp.bfloat16)
    placed = []
    for i in range(8):
        one = jnp.concatenate([jnp.concatenate(ones[2 * i]), jnp.concatenate(ones[2 * i + 1])], axis=1)
        count = jnp.dot(jnp.concatenate([one, before], axis=1), upto, preferred_element_type=jnp.float32)
        before = before + one
        rank = jnp.sum(count * one.astype(jnp.float32), axis=0, keepdims=True) - 1.0
        rank = rank + jnp.concatenate([quarter[2 * i : 2 * i + 1], quarter[2 * i + 1 : 2 * i + 2]], axis=1)
        placed.append(jnp.where(places == rank, 1.0, 0.0).astype(jnp.bfloat16))
    placed = jnp.concatenate(placed, axis=1)
    fours = (spot >> 2).astype(jnp.float32)
    rows = [[jnp.where(spread(fours, i) == sub16 + jnp.bfloat16(16 * k), yes, no) for k in range(2)] for i in range(16)]
    held = []
    for x in pieces:
        held.append(jnp.concatenate([jnp.concatenate([o * spread(x, i) for o in rows[i]]) for i in range(16)], axis=1))
    r = lax.dot_general(
        jnp.concatenate(held), placed, (((1,), (1,)), ((), ())), preferred_element_type=jnp.float32
    )
    r = [r[32 * k : 32 * k + 32] for k in range(7)]
    both = (r[0] + r[1], r[2] + r[3], r[4] * 4096.0 + r[5] * 16.0 + r[6])
    for i in range(16):
        x = i // 4
        for v in range(3):
            out_ref[i, 8 * v : 8 * v + 8, :] = both[v][8 * x : 8 * x + 8]


def buckets(dest, off, vis, interpret=False):
    vmem = pl.BlockSpec(memory_space=pltpu.VMEM)
    return pl.pallas_call(
        bucket_kernel,
        out_shape=jax.ShapeDtypeStruct((16, 24, 128), jnp.float32),
        in_specs=[vmem, vmem, vmem],
        out_specs=vmem,
        interpret=interpret,
    )(dest, off, vis)


def image_kernel(first_ref, *refs):
    own_refs, other_refs, refs = refs[:4], refs[4:8], refs[8:]
    out_ref, p0_ref, p1_ref, q0_ref, q1_ref, h0_ref, h1_ref, y0_ref, y1_ref, sum_ref, dft_ref, vis0_ref, vis1_ref, tw_ref, r_ref, ab_ref = refs
    first = first_ref[0]
    segment = lax.broadcasted_iota(jnp.int32, (16, 128), 1) >> 5
    odd, upper = (segment & 1) == 1, segment >= 2

    def swapped(a, b, mask, by):
        return jnp.where(mask, pltpu.roll(b, by, 1), a), jnp.where(mask, b, pltpu.roll(a, 128 - by, 1))

    def regroup(v, k, plane, vis_ref):
        for half, area in enumerate((own_refs, other_refs)):
            x = [ref[pl.ds(8 * v + 4 * plane + k, 16, stride=24), :] for ref in area]
            x[0], x[1] = swapped(x[0], x[1], odd, 32)
            x[2], x[3] = swapped(x[2], x[3], odd, 32)
            x[0], x[2] = swapped(x[0], x[2], upper, 64)
            x[1], x[3] = swapped(x[1], x[3], upper, 64)
            for j in range(4):
                at = (v * BANDS + 4 * k + j) * GROUPS + 16 * half
                vis_ref[pl.ds(pl.multiple_of(at, 16), 16), :] = x[j]

    def regroup_first(k, c):
        for j in range(2):
            for v in range(3):
                regroup(v, 2 * k + j, 0, vis0_ref)
        return c

    lax.fori_loop(0, 2, regroup_first, 0)

    def values(v, s, vis_ref):
        return vis_ref[pl.ds(pl.multiple_of((v * BANDS + s) * GROUPS, GROUPS), GROUPS), :]

    def make_dft(i):
        k = 2 * (lax.broadcasted_iota(jnp.int32, (16, 256), 0) + 16 * i) + 1
        k = k * lax.broadcasted_iota(jnp.int32, (16, 256), 1) * 16
        for j, x in enumerate(cis_half(k)):
            rows = pl.ds(pl.multiple_of(128 * j + 16 * i, 16), 16)
            hi = x.astype(jnp.bfloat16)
            dft_ref[rows, 0:256] = hi
            dft_ref[rows, 256:512] = (x - hi.astype(jnp.float32)).astype(jnp.bfloat16)
            dft_ref[rows, 512:768] = hi

    def tables(s, vis_ref, p_ref, q_ref):
        off = values(2, s, vis_ref).astype(jnp.int32)
        col = off & (G - 1)
        row = off >> 12
        p_ref[pl.ds(16 * GROUPS, GROUPS), :] = (row & 15).astype(jnp.float32)
        p_ref[pl.ds(17 * GROUPS, GROUPS), :] = (row >> 4).astype(jnp.float32)
        half = cis_half(col)
        one = mul(half, half)
        base = mul((values(0, s, vis_ref), values(1, s, vis_ref)), cis_half(col * (2 * first + 15) - 16 * (row >> 4) - 256 * s))
        power = half
        for k in range(8):
            q_ref[pl.ds(k * SKIP, GROUPS), :] = power[0]
            q_ref[pl.ds((8 + k) * SKIP, GROUPS), :] = power[1]
            if k < 7:
                power = mul(power, one)
        step = one
        for k in range(4):
            step = mul(step, step)
        for k in range(8):
            p_ref[pl.ds(k * GROUPS, GROUPS), :] = base[0]
            p_ref[pl.ds((8 + k) * GROUPS, GROUPS), :] = base[1]
            if k < 7:
                base = mul(base, step)

    sub16 = lax.broadcasted_iota(jnp.int32, (16, 128), 0).astype(jnp.float32).astype(jnp.bfloat16)
    yes = jnp.ones((16, 128), jnp.bfloat16)
    no = jnp.zeros((16, 128), jnp.bfloat16)

    def made(g, p_ref, q_ref):
        def spread(row):
            return jnp.broadcast_to(p_ref[pl.ds(row * GROUPS + g, 1), :], (16, 128)).astype(jnp.bfloat16)

        high = jnp.where(spread(17) == sub16, spread(16), -yes)
        o = [jnp.where(high == jnp.bfloat16(k), yes, no) for k in range(16)]
        qr = q_ref[pl.ds(g, 8, stride=SKIP), :]
        qi = q_ref[pl.ds(8 * SKIP + g, 8, stride=SKIP), :]
        products = []
        for part, q in ((0, qr), (8, qi), (0, qi), (8, qr)):
            for k in range(0, 8, 2):
                two = [p_ref[pl.ds((part + k + j) * GROUPS + g, 1), :] * q for j in range(2)]
                products.append(jnp.concatenate(two).astype(jnp.bfloat16))
        return jnp.concatenate(o), jnp.concatenate(products)

    def phase(used, later, s, h_ref, vis_ref):
        tables(jnp.minimum(s + 1, BANDS - 1), vis_ref, *later)
        parts = [made(g, *used) for g in range(GROUPS)]
        o = jnp.concatenate([x[0] for x in parts], axis=1)
        e = jnp.concatenate([x[1] for x in parts], axis=1)
        part = lax.dot_general(o, e, (((1,), (1,)), ((), ())), preferred_element_type=jnp.float32)
        at = pl.ds(pl.multiple_of(s * 16, 16), 16)
        for k in range(16):
            h_ref[k, at, :] = part[16 * k : 16 * k + 16, :]

    sign = jnp.where(lax.broadcasted_iota(jnp.int32, (256, 128), 1) < 64, -1.0, 1.0)

    def dft(k, h_ref, y_ref):
        re, im = h_ref[k, :, 0:128], h_ref[k, :, 128:256]
        re = re + sign * pltpu.roll(re, 64, 1)
        im = im - sign * pltpu.roll(im, 64, 1)
        x = jnp.concatenate([re, im], axis=1)
        hi = x.astype(jnp.bfloat16)
        lo = (x - hi.astype(jnp.float32)).astype(jnp.bfloat16)
        both = jnp.concatenate([hi, hi, lo], axis=0)
        r = jnp.dot(dft_ref[...], both, preferred_element_type=jnp.float32)
        c_re, c_im, s_re, s_im = r[:128, :128], r[:128, 128:], r[128:, :128], r[128:, 128:]
        y_ref[k, 0:128, 0:128] = c_re - s_im
        y_ref[k, 0:128, 128:256] = c_im + s_re
        y_ref[k, 128:256, 0:128] = c_re + s_im
        y_ref[k, 128:256, 128:256] = c_im - s_re

    place = lax.broadcasted_iota(jnp.int32, (8, 128), 1)
    lower = place & 63
    lane = 2 * (lower - (lower & 7)) + jnp.where(place < 64, 8 + (lower & 7), 7 - (lower & 7))
    inner = place & 15
    source = ((place - inner) >> 1) + jnp.where(inner < 8, 71 - inner, inner - 8)
    lane = lane + first
    sub_row = lax.broadcasted_iota(jnp.int32, (8, 128), 0)
    scale = 0.5 / G
    y = (((lane + 2048) & 4095) - 2048).astype(jnp.float32) * scale
    rest = 1.0 - y * y
    def spread8(row, k):
        return jnp.broadcast_to(row[:, k : k + 1], (8, 128))

    w_row = sum(ref[384:385, :] for ref in own_refs) * 0.5
    taps_row = own_refs[0][385:386, :]

    def twiddles(line):
        tw = [None, cis_int(line)]
        for k in range(2, 16):
            tw.append(mul(tw[k // 2], tw[k - k // 2]))
        return tw

    def half_tile(t, half):
        line = sub_row + t * 8
        return pl.ds(pl.multiple_of(t * 8 + 128 * half, 8), 8), 255 - line if half else line

    def twist(at, k):
        return tw_ref[k - 1, at, :], tw_ref[14 + k, at, :]

    def terms(at, w, y_ref):
        xs = []
        for k in range(16):
            x = (y_ref[k, at, 0:128], y_ref[k, at, 128:256])
            xs.append(x if k == 0 else mul(x, twist(at, k)))
        f = fft(xs)
        result = []
        for j in range(16):
            turn = w * r_ref[j, at, :] - w
            turn = turn - jnp.round(turn)
            result.append(mul(f[j], cis4(turn)))
        return result

    taps = [spread8(taps_row, k) for k in range(8)]
    step = cis_int(lane)
    weight = [x.astype(jnp.bfloat16).astype(jnp.float32) * (1.0 / 512) for x in taps]
    b = (weight[7], jnp.zeros((8, 128), jnp.float32))
    for k in range(6, -1, -1):
        b = mul(b, step)
        b = (b[0] + weight[k], b[1])

    def prepare(t):
        for half in range(2):
            at, line = half_tile(t, half)
            tw = twiddles(line)
            for k in range(1, 16):
                tw_ref[k - 1, at, :] = tw[k][0]
                tw_ref[14 + k, at, :] = tw[k][1]
            ts = [(taps[0], jnp.zeros((8, 128), jnp.float32))]
            ts += [(tw[k][0] * taps[k], tw[k][1] * taps[k]) for k in range(1, 8)]
            a = fft(ts + [None] * 8)
            x0 = line.astype(jnp.float32) * scale
            for j in range(16):
                x = x0 + (256 * j if j < 8 else 256 * j - G) * scale
                z = rest - x * x
                r_ref[j, at, :] = z * lax.rsqrt(z)
                ab = mul(a[j], b)
                ab_ref[2 * j, at, :] = ab[0]
                ab_ref[2 * j + 1, at, :] = ab[1]

    buf0, buf1 = (p0_ref, q0_ref), (p1_ref, q1_ref)
    tables(0, vis0_ref, *buf0)

    def sets_of_first(i, c):
        for k in range(0, 4, 2):
            phase(buf0, buf1, 4 * i + k, h0_ref, vis0_ref)
            phase(buf1, buf0, 4 * i + k + 1, h0_ref, vis0_ref)
            make_dft(2 * i + k // 2)
            prepare(2 * i + k // 2)
        for v in range(3):
            regroup(v, i, 1, vis1_ref)
        return c

    lax.fori_loop(0, 4, sets_of_first, 0)
    tables(0, vis1_ref, *buf0)

    def sets_of_second(i, c):
        for k in range(0, 4, 2):
            phase(buf0, buf1, 4 * i + k, h1_ref, vis1_ref)
            dft(4 * i + k, h0_ref, y0_ref)
            phase(buf1, buf0, 4 * i + k + 1, h1_ref, vis1_ref)
            dft(4 * i + k + 1, h0_ref, y0_ref)
            prepare(8 + 2 * i + k // 2)
        return c

    lax.fori_loop(0, 4, sets_of_second, 0)
    w0 = spread8(w_row, 0)

    def tiles_of_first(i, c):
        for k in range(STEPS):
            dft(STEPS * i + k, h1_ref, y1_ref)
        for k in range(STEPS):
            for half in range(2):
                at, _ = half_tile(STEPS * i + k, half)
                for j, x in enumerate(terms(at, w0, y0_ref)):
                    sum_ref[j, at, 0:128] = x[0]
                    sum_ref[j, at, 128:256] = x[1]
        return c

    lax.fori_loop(0, 16 // STEPS, tiles_of_first, 0)
    w1 = spread8(w_row, 1)

    def tiles_of_second(t, c):
        for half in range(2):
            at, _ = half_tile(t, half)
            place = pl.ds(pl.multiple_of(248 - t * 8 if half else t * 8, 8), 8)
            for j, x in enumerate(terms(at, w1, y1_ref)):
                x = add(x, (sum_ref[j, at, 0:128], sum_ref[j, at, 128:256]))
                pixel = x[0] * ab_ref[2 * j, at, :] - x[1] * ab_ref[2 * j + 1, at, :]
                pixel = jnp.take_along_axis(pixel, source, axis=1)
                if half:
                    pixel = jnp.take_along_axis(pixel, 7 - sub_row, axis=0)
                out_ref[j, place, :] = pixel
        return c

    lax.fori_loop(0, 16, tiles_of_second, 0)


def part_image(first, *area, interpret=False):
    smem = pl.BlockSpec(memory_space=pltpu.SMEM)
    vmem = pl.BlockSpec(memory_space=pltpu.VMEM)
    return pl.pallas_call(
        image_kernel,
        out_shape=jax.ShapeDtypeStruct((16, 256, COLS), jnp.float32),
        in_specs=[smem] + [vmem] * 8,
        out_specs=vmem,
        scratch_shapes=[
            pltpu.VMEM((18 * GROUPS, 128), jnp.float32),
            pltpu.VMEM((18 * GROUPS, 128), jnp.float32),
            pltpu.VMEM((16 * SKIP, 128), jnp.float32),
            pltpu.VMEM((16 * SKIP, 128), jnp.float32),
            pltpu.VMEM((16, 256, 256), jnp.float32),
            pltpu.VMEM((16, 256, 256), jnp.float32),
            pltpu.VMEM((16, 256, 256), jnp.float32),
            pltpu.VMEM((16, 256, 256), jnp.float32),
            pltpu.VMEM((16, 256, 256), jnp.float32),
            pltpu.VMEM((256, 768), jnp.bfloat16),
            pltpu.VMEM((3 * BANDS * GROUPS, 128), jnp.float32),
            pltpu.VMEM((3 * BANDS * GROUPS, 128), jnp.float32),
            pltpu.VMEM((30, 256, 128), jnp.float32),
            pltpu.VMEM((16, 256, 128), jnp.float32),
            pltpu.VMEM((32, 256, 128), jnp.float32),
        ],
        compiler_params=pltpu.CompilerParams(vmem_limit_bytes=56 * 1024 * 1024),
        interpret=interpret,
    )(first, *area)


def shifted(x, axis, by):
    length = lax.axis_size(axis)
    return lax.ppermute(x, axis, [(i, (i + by) % length) for i in range(length)])


def local(visibility, target, offset, taps, w_plane):
    half = lax.axis_index("plane_0")
    out = buckets(target.reshape(1, 2048), offset.reshape(16, 128), visibility)
    own = lax.all_to_all(out, ("plane_1", "tile_1"), split_axis=0, concat_axis=0, tiled=True).reshape(384, 128)
    w_row = jnp.where(jnp.arange(128) == half, w_plane[0], 0.0)
    own = jnp.concatenate([own, w_row[None], jnp.pad(taps, (0, 120))[None], jnp.zeros((6, 128), jnp.float32)])
    area = [own] + [shifted(own, ("plane_0", "tile_0"), by) for by in (1, 2, 3)]
    area = area + [shifted(x, "tile_2", 1) for x in area]
    first = lax.axis_index(TILE) * 256 + half * COLS
    first = first.reshape(1).astype(jnp.int32)
    part = part_image(first, *area).reshape(G, COLS)
    arrived = lax.all_to_all(part, PLANE, split_axis=0, concat_axis=0, tiled=True)
    total = arrived.reshape(2, 4, 512, COLS).sum(axis=1)
    return jnp.concatenate([total[0], total[1]], axis=1)


def solution(mesh):
    finer = Mesh(
        mesh.devices.reshape(2, 4, 2, 4, 2), ("plane_0", "plane_1", "tile_0", "tile_1", "tile_2")
    )
    return jax.shard_map(
        local,
        mesh=finer,
        in_specs=(P(None, PLANE_TILE), P(PLANE_TILE, None), P(PLANE_TILE), P(), P(PLANE)),
        out_specs=P(PLANE, TILE),
        check_vma=False,
    )
```

```python
import math

import jax
import jax.numpy as jnp
import numpy as np
from jax import lax
from jax.experimental import pallas as pl
from jax.experimental.pallas import tpu as pltpu
from jax.sharding import Mesh
from jax.sharding import PartitionSpec as P

G = 4096
TILE = ("tile_0", "tile_1", "tile_2")
PLANE = ("plane_0", "plane_1")
PLANE_TILE = PLANE + TILE
BANDS = 16
CAP = 32
PAIR = 2
COLS = 128
SETS = PAIR * BANDS
SKIP = 33
STEPS = 4
GROUPS = 32

SIN = (6.283183359351797, -41.341456456971535, 81.59688036372165, -76.58598132852413,
       41.227609837804344, -12.302204294679466)
COS = (0.9999996601928737, -19.739032170917408, 64.93001305163173, -85.28516993938109,
       58.84794870978477, -21.158227293307913)


SIN4 = (6.283080178478066, -41.332270740282254, 81.3803723363611, -74.5450983459368, 32.89453310276785)
COS4 = (0.9999814280910587, -19.732589155128917, 64.69856260154607, -82.54685792407774, 45.912495330496334)


def horner(u, coefs):
    total = jnp.full_like(u, coefs[-1])
    for c in coefs[-2::-1]:
        total = total * u + c
    return total


def cis(turn):
    u = turn * turn
    return horner(u, COS), turn * horner(u, SIN)


def cis4(turn):
    u = turn * turn
    return horner(u, COS4), turn * horner(u, SIN4)


def cis_int(k):
    return cis((((k + 2048) & 4095) - 2048).astype(jnp.float32) * (1.0 / 4096))


def cis_half(k):
    return cis((((k + 4096) & 8191) - 4096).astype(jnp.float32) * (1.0 / 8192))


def mul(a, b):
    return a[0] * b[0] - a[1] * b[1], a[0] * b[1] + a[1] * b[0]


def add(a, b):
    if b is None:
        return a
    return a[0] + b[0], a[1] + b[1]


def sub(a, b):
    if b is None:
        return a
    return a[0] - b[0], a[1] - b[1]


def turned(a, k, n):
    k = k % n
    if a is None or k == 0:
        return a
    if 4 * k == n:
        return -a[1], a[0]
    if 8 * k == n:
        h = math.sqrt(0.5)
        return (a[0] - a[1]) * h, (a[0] + a[1]) * h
    if 8 * k == 3 * n:
        h = math.sqrt(0.5)
        return (-a[0] - a[1]) * h, (a[0] - a[1]) * h
    c, s = math.cos(2 * math.pi * k / n), math.sin(2 * math.pi * k / n)
    return a[0] * c - a[1] * s, a[0] * s + a[1] * c


def fft(xs):
    n = len(xs)
    if n == 1:
        return xs
    even, odd = fft(xs[0::2]), fft(xs[1::2])
    odd = [turned(o, k, n) for k, o in enumerate(odd)]
    return [add(e, o) for e, o in zip(even, odd)] + [sub(e, o) for e, o in zip(even, odd)]


def bucket_kernel(dest_ref, off_ref, vis_ref, out_ref):
    dest = jnp.concatenate([dest_ref[0:1, 128 * i : 128 * i + 128] for i in range(16)])
    plane, band = dest >> 4, dest & 15
    spot = ((plane & 3) * 2 + (plane >> 2)) * BANDS + band
    low, high = (spot & 15).astype(jnp.float32), (spot >> 4).astype(jnp.float32)
    off = off_ref[...]
    pieces = []
    for v in range(2):
        x = jnp.concatenate([vis_ref[v : v + 1, 128 * i : 128 * i + 128] for i in range(16)])
        top = x.astype(jnp.bfloat16).astype(jnp.float32)
        pieces += [top, x - top]
    pieces += [(off >> 12).astype(jnp.float32), ((off >> 4) & 255).astype(jnp.float32), (off & 15).astype(jnp.float32)]
    sub16 = lax.broadcasted_iota(jnp.int32, (16, 128), 0).astype(jnp.float32).astype(jnp.bfloat16)
    yes, no = jnp.ones((16, 128), jnp.bfloat16), jnp.zeros((16, 128), jnp.bfloat16)
    first = lax.broadcasted_iota(jnp.int32, (256, 256), 0) <= lax.broadcasted_iota(jnp.int32, (256, 256), 1)
    upto = jnp.where(first, 1.0, 0.0).astype(jnp.bfloat16)
    upto = jnp.concatenate([upto, jnp.ones((256, 256), jnp.bfloat16)])

    def spread(x, i):
        return jnp.broadcast_to(x[i : i + 1], (16, 128)).astype(jnp.bfloat16)

    ones = []
    for i in range(16):
        code = jnp.where(spread(low, i) == sub16, spread(high, i), -yes)
        ones.append([jnp.where(code == jnp.bfloat16(k), yes, no) for k in range(8)])
    quarter = ((spot & 3) * CAP).astype(jnp.float32)
    places = lax.broadcasted_iota(jnp.int32, (128, 256), 0).astype(jnp.float32)
    before = jnp.zeros((128, 256), jnp.bfloat16)
    placed = []
    for i in range(8):
        one = jnp.concatenate([jnp.concatenate(ones[2 * i]), jnp.concatenate(ones[2 * i + 1])], axis=1)
        count = jnp.dot(jnp.concatenate([one, before], axis=1), upto, preferred_element_type=jnp.float32)
        before = before + one
        rank = jnp.sum(count * one.astype(jnp.float32), axis=0, keepdims=True) - 1.0
        rank = rank + jnp.concatenate([quarter[2 * i : 2 * i + 1], quarter[2 * i + 1 : 2 * i + 2]], axis=1)
        placed.append(jnp.where(places == rank, 1.0, 0.0).astype(jnp.bfloat16))
    placed = jnp.concatenate(placed, axis=1)
    fours = (spot >> 2).astype(jnp.float32)
    rows = [[jnp.where(spread(fours, i) == sub16 + jnp.bfloat16(16 * k), yes, no) for k in range(2)] for i in range(16)]
    held = []
    for x in pieces:
        held.append(jnp.concatenate([jnp.concatenate([o * spread(x, i) for o in rows[i]]) for i in range(16)], axis=1))
    r = lax.dot_general(
        jnp.concatenate(held), placed, (((1,), (1,)), ((), ())), preferred_element_type=jnp.float32
    )
    r = [r[32 * k : 32 * k + 32] for k in range(7)]
    both = (r[0] + r[1], r[2] + r[3], r[4] * 4096.0 + r[5] * 16.0 + r[6])
    for i in range(16):
        x = i % 4
        for v in range(3):
            out_ref[i, 8 * v : 8 * v + 8, :] = both[v][8 * x : 8 * x + 8]


def buckets(dest, off, vis, interpret=False):
    vmem = pl.BlockSpec(memory_space=pltpu.VMEM)
    return pl.pallas_call(
        bucket_kernel,
        out_shape=jax.ShapeDtypeStruct((16, 24, 128), jnp.float32),
        in_specs=[vmem, vmem, vmem],
        out_specs=vmem,
        interpret=interpret,
    )(dest, off, vis)


def image_kernel(first_ref, *refs):
    own_refs, other_refs, refs = refs[:4], refs[4:8], refs[8:]
    out_ref, p0_ref, p1_ref, q0_ref, q1_ref, h0_ref, h1_ref, y0_ref, y1_ref, sum_ref, dft_ref, vis0_ref, vis1_ref, tw_ref, r_ref, ab_ref = refs
    first = first_ref[0]
    segment = lax.broadcasted_iota(jnp.int32, (16, 128), 1) >> 5
    odd, upper = (segment & 1) == 1, segment >= 2

    def swapped(a, b, mask, by):
        return jnp.where(mask, pltpu.roll(b, by, 1), a), jnp.where(mask, b, pltpu.roll(a, 128 - by, 1))

    def regroup(v, k, plane, vis_ref):
        for half, area in enumerate((own_refs, other_refs)):
            x = [ref[pl.ds(8 * v + 4 * plane + k, 16, stride=24), :] for ref in area]
            x[0], x[1] = swapped(x[0], x[1], odd, 32)
            x[2], x[3] = swapped(x[2], x[3], odd, 32)
            x[0], x[2] = swapped(x[0], x[2], upper, 64)
            x[1], x[3] = swapped(x[1], x[3], upper, 64)
            for j in range(4):
                at = (v * BANDS + 4 * k + j) * GROUPS + 16 * half
                vis_ref[pl.ds(pl.multiple_of(at, 16), 16), :] = x[j]

    def regroup_first(k, c):
        for j in range(2):
            for v in range(3):
                regroup(v, 2 * k + j, 0, vis0_ref)
        return c

    lax.fori_loop(0, 2, regroup_first, 0)

    def values(v, s, vis_ref):
        return vis_ref[pl.ds(pl.multiple_of((v * BANDS + s) * GROUPS, GROUPS), GROUPS), :]

    def make_dft(i):
        k = 2 * (lax.broadcasted_iota(jnp.int32, (16, 256), 0) + 16 * i) + 1
        k = k * lax.broadcasted_iota(jnp.int32, (16, 256), 1) * 16
        for j, x in enumerate(cis_half(k)):
            rows = pl.ds(pl.multiple_of(128 * j + 16 * i, 16), 16)
            hi = x.astype(jnp.bfloat16)
            dft_ref[rows, 0:256] = hi
            dft_ref[rows, 256:512] = (x - hi.astype(jnp.float32)).astype(jnp.bfloat16)
            dft_ref[rows, 512:768] = hi

    def tables(s, vis_ref, p_ref, q_ref):
        off = values(2, s, vis_ref).astype(jnp.int32)
        col = off & (G - 1)
        row = off >> 12
        p_ref[pl.ds(16 * GROUPS, GROUPS), :] = (row & 15).astype(jnp.float32)
        p_ref[pl.ds(17 * GROUPS, GROUPS), :] = (row >> 4).astype(jnp.float32)
        half = cis_half(col)
        one = mul(half, half)
        base = mul((values(0, s, vis_ref), values(1, s, vis_ref)), cis_half(col * (2 * first + 15) - 16 * (row >> 4) - 256 * s))
        power = half
        for k in range(8):
            q_ref[pl.ds(k * SKIP, GROUPS), :] = power[0]
            q_ref[pl.ds((8 + k) * SKIP, GROUPS), :] = power[1]
            if k < 7:
                power = mul(power, one)
        step = one
        for k in range(4):
            step = mul(step, step)
        for k in range(8):
            p_ref[pl.ds(k * GROUPS, GROUPS), :] = base[0]
            p_ref[pl.ds((8 + k) * GROUPS, GROUPS), :] = base[1]
            if k < 7:
                base = mul(base, step)

    sub16 = lax.broadcasted_iota(jnp.int32, (16, 128), 0).astype(jnp.float32).astype(jnp.bfloat16)
    yes = jnp.ones((16, 128), jnp.bfloat16)
    no = jnp.zeros((16, 128), jnp.bfloat16)

    def made(g, p_ref, q_ref):
        def spread(row):
            return jnp.broadcast_to(p_ref[pl.ds(row * GROUPS + g, 1), :], (16, 128)).astype(jnp.bfloat16)

        high = jnp.where(spread(17) == sub16, spread(16), -yes)
        o = [jnp.where(high == jnp.bfloat16(k), yes, no) for k in range(16)]
        qr = q_ref[pl.ds(g, 8, stride=SKIP), :]
        qi = q_ref[pl.ds(8 * SKIP + g, 8, stride=SKIP), :]
        products = []
        for part, q in ((0, qr), (8, qi), (0, qi), (8, qr)):
            for k in range(0, 8, 2):
                two = [p_ref[pl.ds((part + k + j) * GROUPS + g, 1), :] * q for j in range(2)]
                products.append(jnp.concatenate(two).astype(jnp.bfloat16))
        return jnp.concatenate(o), jnp.concatenate(products)

    def phase(used, later, s, h_ref, vis_ref):
        tables(jnp.minimum(s + 1, BANDS - 1), vis_ref, *later)
        parts = [made(g, *used) for g in range(GROUPS)]
        o = jnp.concatenate([x[0] for x in parts], axis=1)
        e = jnp.concatenate([x[1] for x in parts], axis=1)
        part = lax.dot_general(o, e, (((1,), (1,)), ((), ())), preferred_element_type=jnp.float32)
        at = pl.ds(pl.multiple_of(s * 16, 16), 16)
        for k in range(16):
            h_ref[k, at, :] = part[16 * k : 16 * k + 16, :]

    sign = jnp.where(lax.broadcasted_iota(jnp.int32, (256, 128), 1) < 64, -1.0, 1.0)

    def dft(k, h_ref, y_ref):
        re, im = h_ref[k, :, 0:128], h_ref[k, :, 128:256]
        re = re + sign * pltpu.roll(re, 64, 1)
        im = im - sign * pltpu.roll(im, 64, 1)
        x = jnp.concatenate([re, im], axis=1)
        hi = x.astype(jnp.bfloat16)
        lo = (x - hi.astype(jnp.float32)).astype(jnp.bfloat16)
        both = jnp.concatenate([hi, hi, lo], axis=0)
        r = jnp.dot(dft_ref[...], both, preferred_element_type=jnp.float32)
        c_re, c_im, s_re, s_im = r[:128, :128], r[:128, 128:], r[128:, :128], r[128:, 128:]
        y_ref[k, 0:128, 0:128] = c_re - s_im
        y_ref[k, 0:128, 128:256] = c_im + s_re
        y_ref[k, 128:256, 0:128] = c_re + s_im
        y_ref[k, 128:256, 128:256] = c_im - s_re

    place = lax.broadcasted_iota(jnp.int32, (8, 128), 1)
    lower = place & 63
    lane = 2 * (lower - (lower & 7)) + jnp.where(place < 64, 8 + (lower & 7), 7 - (lower & 7))
    inner = place & 15
    source = ((place - inner) >> 1) + jnp.where(inner < 8, 71 - inner, inner - 8)
    lane = lane + first
    sub_row = lax.broadcasted_iota(jnp.int32, (8, 128), 0)
    scale = 0.5 / G
    y = (((lane + 2048) & 4095) - 2048).astype(jnp.float32) * scale
    rest = 1.0 - y * y
    def spread8(row, k):
        return jnp.broadcast_to(row[:, k : k + 1], (8, 128))

    w_row = sum(ref[384:385, :] for ref in own_refs) * 0.5
    taps_row = own_refs[0][385:386, :]

    def twiddles(line):
        tw = [None, cis_int(line)]
        for k in range(2, 16):
            tw.append(mul(tw[k // 2], tw[k - k // 2]))
        return tw

    def half_tile(t, half):
        line = sub_row + t * 8
        return pl.ds(pl.multiple_of(t * 8 + 128 * half, 8), 8), 255 - line if half else line

    def twist(at, k):
        return tw_ref[k - 1, at, :], tw_ref[14 + k, at, :]

    def terms(at, w, y_ref):
        xs = []
        for k in range(16):
            x = (y_ref[k, at, 0:128], y_ref[k, at, 128:256])
            xs.append(x if k == 0 else mul(x, twist(at, k)))
        f = fft(xs)
        result = []
        for j in range(16):
            turn = w * r_ref[j, at, :] - w
            turn = turn - jnp.round(turn)
            result.append(mul(f[j], cis4(turn)))
        return result

    taps = [spread8(taps_row, k) for k in range(8)]
    step = cis_int(lane)
    weight = [x.astype(jnp.bfloat16).astype(jnp.float32) * (1.0 / 512) for x in taps]
    b = (weight[7], jnp.zeros((8, 128), jnp.float32))
    for k in range(6, -1, -1):
        b = mul(b, step)
        b = (b[0] + weight[k], b[1])

    def prepare(t):
        for half in range(2):
            at, line = half_tile(t, half)
            tw = twiddles(line)
            for k in range(1, 16):
                tw_ref[k - 1, at, :] = tw[k][0]
                tw_ref[14 + k, at, :] = tw[k][1]
            ts = [(taps[0], jnp.zeros((8, 128), jnp.float32))]
            ts += [(tw[k][0] * taps[k], tw[k][1] * taps[k]) for k in range(1, 8)]
            a = fft(ts + [None] * 8)
            x0 = line.astype(jnp.float32) * scale
            for j in range(16):
                x = x0 + (256 * j if j < 8 else 256 * j - G) * scale
                z = rest - x * x
                r_ref[j, at, :] = z * lax.rsqrt(z)
                ab = mul(a[j], b)
                ab_ref[2 * j, at, :] = ab[0]
                ab_ref[2 * j + 1, at, :] = ab[1]

    buf0, buf1 = (p0_ref, q0_ref), (p1_ref, q1_ref)
    tables(0, vis0_ref, *buf0)

    def sets_of_first(i, c):
        for k in range(0, 4, 2):
            phase(buf0, buf1, 4 * i + k, h0_ref, vis0_ref)
            phase(buf1, buf0, 4 * i + k + 1, h0_ref, vis0_ref)
            make_dft(2 * i + k // 2)
            prepare(2 * i + k // 2)
        for v in range(3):
            regroup(v, i, 1, vis1_ref)
        return c

    lax.fori_loop(0, 4, sets_of_first, 0)
    tables(0, vis1_ref, *buf0)

    def sets_of_second(i, c):
        for k in range(0, 4, 2):
            phase(buf0, buf1, 4 * i + k, h1_ref, vis1_ref)
            dft(4 * i + k, h0_ref, y0_ref)
            phase(buf1, buf0, 4 * i + k + 1, h1_ref, vis1_ref)
            dft(4 * i + k + 1, h0_ref, y0_ref)
            prepare(8 + 2 * i + k // 2)
        return c

    lax.fori_loop(0, 4, sets_of_second, 0)
    w0 = spread8(w_row, 0)

    def tiles_of_first(i, c):
        for k in range(STEPS):
            dft(STEPS * i + k, h1_ref, y1_ref)
        for k in range(STEPS):
            for half in range(2):
                at, _ = half_tile(STEPS * i + k, half)
                for j, x in enumerate(terms(at, w0, y0_ref)):
                    sum_ref[j, at, 0:128] = x[0]
                    sum_ref[j, at, 128:256] = x[1]
        return c

    lax.fori_loop(0, 16 // STEPS, tiles_of_first, 0)
    w1 = spread8(w_row, 1)

    def tiles_of_second(t, c):
        for half in range(2):
            at, _ = half_tile(t, half)
            place = pl.ds(pl.multiple_of(248 - t * 8 if half else t * 8, 8), 8)
            for j, x in enumerate(terms(at, w1, y1_ref)):
                x = add(x, (sum_ref[j, at, 0:128], sum_ref[j, at, 128:256]))
                pixel = x[0] * ab_ref[2 * j, at, :] - x[1] * ab_ref[2 * j + 1, at, :]
                pixel = jnp.take_along_axis(pixel, source, axis=1)
                if half:
                    pixel = jnp.take_along_axis(pixel, 7 - sub_row, axis=0)
                out_ref[4 * (j // 2 % 4) + 2 * (j // 8) + j % 2, place, :] = pixel
        return c

    lax.fori_loop(0, 16, tiles_of_second, 0)


def part_image(first, *area, interpret=False):
    smem = pl.BlockSpec(memory_space=pltpu.SMEM)
    vmem = pl.BlockSpec(memory_space=pltpu.VMEM)
    return pl.pallas_call(
        image_kernel,
        out_shape=jax.ShapeDtypeStruct((16, 256, COLS), jnp.float32),
        in_specs=[smem] + [vmem] * 8,
        out_specs=vmem,
        scratch_shapes=[
            pltpu.VMEM((18 * GROUPS, 128), jnp.float32),
            pltpu.VMEM((18 * GROUPS, 128), jnp.float32),
            pltpu.VMEM((16 * SKIP, 128), jnp.float32),
            pltpu.VMEM((16 * SKIP, 128), jnp.float32),
            pltpu.VMEM((16, 256, 256), jnp.float32),
            pltpu.VMEM((16, 256, 256), jnp.float32),
            pltpu.VMEM((16, 256, 256), jnp.float32),
            pltpu.VMEM((16, 256, 256), jnp.float32),
            pltpu.VMEM((16, 256, 256), jnp.float32),
            pltpu.VMEM((256, 768), jnp.bfloat16),
            pltpu.VMEM((3 * BANDS * GROUPS, 128), jnp.float32),
            pltpu.VMEM((3 * BANDS * GROUPS, 128), jnp.float32),
            pltpu.VMEM((30, 256, 128), jnp.float32),
            pltpu.VMEM((16, 256, 128), jnp.float32),
            pltpu.VMEM((32, 256, 128), jnp.float32),
        ],
        compiler_params=pltpu.CompilerParams(vmem_limit_bytes=56 * 1024 * 1024),
        interpret=interpret,
    )(first, *area)


def shifted(x, axis, by):
    length = lax.axis_size(axis)
    return lax.ppermute(x, axis, [(i, (i + by) % length) for i in range(length)])


def local(visibility, target, offset, taps, w_plane):
    half = lax.axis_index("plane_0")
    out = buckets(target.reshape(1, 2048), offset.reshape(16, 128), visibility)
    own = lax.all_to_all(out, ("tile_1", "plane_1"), split_axis=0, concat_axis=0, tiled=True).reshape(384, 128)
    w_row = jnp.where(jnp.arange(128) == half, w_plane[0], 0.0)
    own = jnp.concatenate([own, w_row[None], jnp.pad(taps, (0, 120))[None], jnp.zeros((6, 128), jnp.float32)])
    area = [own] + [shifted(own, ("plane_0", "tile_0"), by) for by in (1, 2, 3)]
    area = area + [shifted(x, "tile_2", 1) for x in area]
    first = lax.axis_index(TILE) * 256 + half * COLS
    first = first.reshape(1).astype(jnp.int32)
    part = part_image(first, *area).reshape(G, COLS)
    arrived = lax.all_to_all(part, PLANE[::-1], split_axis=0, concat_axis=0, tiled=True)
    total = arrived.reshape(4, 2, 512, COLS).sum(axis=0)
    return jnp.concatenate([total[0], total[1]], axis=1)


def solution(mesh):
    finer = Mesh(
        mesh.devices.reshape(2, 4, 2, 4, 2), ("plane_0", "plane_1", "tile_0", "tile_1", "tile_2")
    )
    return jax.shard_map(
        local,
        mesh=finer,
        in_specs=(P(None, PLANE_TILE), P(PLANE_TILE, None), P(PLANE_TILE), P(), P(PLANE)),
        out_specs=P(PLANE, TILE),
        check_vma=False,
    )
```

```python
import math

import jax
import jax.numpy as jnp
import numpy as np
from jax import lax
from jax.experimental import pallas as pl
from jax.experimental.pallas import tpu as pltpu
from jax.sharding import Mesh
from jax.sharding import PartitionSpec as P

G = 4096
TILE = ("tile_0", "tile_1", "tile_2")
PLANE = ("plane_0", "plane_1")
PLANE_TILE = PLANE + TILE
BANDS = 16
CAP = 32
PAIR = 2
COLS = 128
SETS = PAIR * BANDS
SKIP = 33
STEPS = 4
GROUPS = 32

SIN = (6.283183359351797, -41.341456456971535, 81.59688036372165, -76.58598132852413,
       41.227609837804344, -12.302204294679466)
COS = (0.9999996601928737, -19.739032170917408, 64.93001305163173, -85.28516993938109,
       58.84794870978477, -21.158227293307913)


SIN4 = (6.283080178478066, -41.332270740282254, 81.3803723363611, -74.5450983459368, 32.89453310276785)
COS4 = (0.9999814280910587, -19.732589155128917, 64.69856260154607, -82.54685792407774, 45.912495330496334)


def horner(u, coefs):
    total = jnp.full_like(u, coefs[-1])
    for c in coefs[-2::-1]:
        total = total * u + c
    return total


def cis(turn):
    u = turn * turn
    return horner(u, COS), turn * horner(u, SIN)


def cis4(turn):
    u = turn * turn
    return horner(u, COS4), turn * horner(u, SIN4)


def cis_int(k):
    return cis((((k + 2048) & 4095) - 2048).astype(jnp.float32) * (1.0 / 4096))


def cis_half(k):
    return cis((((k + 4096) & 8191) - 4096).astype(jnp.float32) * (1.0 / 8192))


def mul(a, b):
    return a[0] * b[0] - a[1] * b[1], a[0] * b[1] + a[1] * b[0]


def add(a, b):
    if b is None:
        return a
    return a[0] + b[0], a[1] + b[1]


def sub(a, b):
    if b is None:
        return a
    return a[0] - b[0], a[1] - b[1]


def turned(a, k, n):
    k = k % n
    if a is None or k == 0:
        return a
    if 4 * k == n:
        return -a[1], a[0]
    if 8 * k == n:
        h = math.sqrt(0.5)
        return (a[0] - a[1]) * h, (a[0] + a[1]) * h
    if 8 * k == 3 * n:
        h = math.sqrt(0.5)
        return (-a[0] - a[1]) * h, (a[0] - a[1]) * h
    c, s = math.cos(2 * math.pi * k / n), math.sin(2 * math.pi * k / n)
    return a[0] * c - a[1] * s, a[0] * s + a[1] * c


def fft(xs):
    n = len(xs)
    if n == 1:
        return xs
    even, odd = fft(xs[0::2]), fft(xs[1::2])
    odd = [turned(o, k, n) for k, o in enumerate(odd)]
    return [add(e, o) for e, o in zip(even, odd)] + [sub(e, o) for e, o in zip(even, odd)]


def bucket_kernel(dest_ref, off_ref, vis_ref, out_ref):
    dest = jnp.concatenate([dest_ref[0:1, 128 * i : 128 * i + 128] for i in range(16)])
    plane, band = dest >> 4, dest & 15
    spot = ((plane & 3) * 2 + (plane >> 2)) * BANDS + band
    low, high = (spot & 15).astype(jnp.float32), (spot >> 4).astype(jnp.float32)
    off = off_ref[...]
    pieces = []
    for v in range(2):
        x = jnp.concatenate([vis_ref[v : v + 1, 128 * i : 128 * i + 128] for i in range(16)])
        top = x.astype(jnp.bfloat16).astype(jnp.float32)
        pieces += [top, x - top]
    pieces += [(off >> 12).astype(jnp.float32), ((off >> 4) & 255).astype(jnp.float32), (off & 15).astype(jnp.float32)]
    sub16 = lax.broadcasted_iota(jnp.int32, (16, 128), 0).astype(jnp.float32).astype(jnp.bfloat16)
    yes, no = jnp.ones((16, 128), jnp.bfloat16), jnp.zeros((16, 128), jnp.bfloat16)
    first = lax.broadcasted_iota(jnp.int32, (256, 256), 0) <= lax.broadcasted_iota(jnp.int32, (256, 256), 1)
    upto = jnp.where(first, 1.0, 0.0).astype(jnp.bfloat16)
    upto = jnp.concatenate([upto, jnp.ones((256, 256), jnp.bfloat16)])

    def spread(x, i):
        return jnp.broadcast_to(x[i : i + 1], (16, 128)).astype(jnp.bfloat16)

    ones = []
    for i in range(16):
        code = jnp.where(spread(low, i) == sub16, spread(high, i), -yes)
        ones.append([jnp.where(code == jnp.bfloat16(k), yes, no) for k in range(8)])
    quarter = ((spot & 3) * CAP).astype(jnp.float32)
    places = lax.broadcasted_iota(jnp.int32, (128, 256), 0).astype(jnp.float32)
    before = jnp.zeros((128, 256), jnp.bfloat16)
    placed = []
    for i in range(8):
        one = jnp.concatenate([jnp.concatenate(ones[2 * i]), jnp.concatenate(ones[2 * i + 1])], axis=1)
        count = jnp.dot(jnp.concatenate([one, before], axis=1), upto, preferred_element_type=jnp.float32)
        before = before + one
        rank = jnp.sum(count * one.astype(jnp.float32), axis=0, keepdims=True) - 1.0
        rank = rank + jnp.concatenate([quarter[2 * i : 2 * i + 1], quarter[2 * i + 1 : 2 * i + 2]], axis=1)
        placed.append(jnp.where(places == rank, 1.0, 0.0).astype(jnp.bfloat16))
    placed = jnp.concatenate(placed, axis=1)
    fours = (spot >> 2).astype(jnp.float32)
    rows = [[jnp.where(spread(fours, i) == sub16 + jnp.bfloat16(16 * k), yes, no) for k in range(2)] for i in range(16)]
    held = []
    for x in pieces:
        held.append(jnp.concatenate([jnp.concatenate([o * spread(x, i) for o in rows[i]]) for i in range(16)], axis=1))
    r = lax.dot_general(
        jnp.concatenate(held), placed, (((1,), (1,)), ((), ())), preferred_element_type=jnp.float32
    )
    r = [r[32 * k : 32 * k + 32] for k in range(7)]
    both = (r[0] + r[1], r[2] + r[3], r[4] * 4096.0 + r[5] * 16.0 + r[6])
    for i in range(16):
        x = i % 4
        for v in range(3):
            out_ref[i, 8 * v : 8 * v + 8, :] = both[v][8 * x : 8 * x + 8]


def buckets(dest, off, vis, interpret=False):
    vmem = pl.BlockSpec(memory_space=pltpu.VMEM)
    return pl.pallas_call(
        bucket_kernel,
        out_shape=jax.ShapeDtypeStruct((16, 24, 128), jnp.float32),
        in_specs=[vmem, vmem, vmem],
        out_specs=vmem,
        interpret=interpret,
    )(dest, off, vis)


def image_kernel(first_ref, *refs):
    own_refs, other_refs, refs = refs[:4], refs[4:8], refs[8:]
    out_ref, p0_ref, p1_ref, q0_ref, q1_ref, h0_ref, h1_ref, y0_ref, y1_ref, sum_ref, dft_ref, vis0_ref, vis1_ref, tw_ref, r_ref, ab_ref = refs
    first = first_ref[0]
    segment = lax.broadcasted_iota(jnp.int32, (16, 128), 1) >> 5
    odd, upper = (segment & 1) == 1, segment >= 2

    def swapped(a, b, mask, by):
        return jnp.where(mask, pltpu.roll(b, by, 1), a), jnp.where(mask, b, pltpu.roll(a, 128 - by, 1))

    def regroup(v, k, plane, vis_ref):
        for half, area in enumerate((own_refs, other_refs)):
            x = [ref[pl.ds(8 * v + 4 * plane + k, 16, stride=24), :] for ref in area]
            x[0], x[1] = swapped(x[0], x[1], odd, 32)
            x[2], x[3] = swapped(x[2], x[3], odd, 32)
            x[0], x[2] = swapped(x[0], x[2], upper, 64)
            x[1], x[3] = swapped(x[1], x[3], upper, 64)
            for j in range(4):
                at = (v * BANDS + 4 * k + j) * GROUPS + 16 * half
                vis_ref[pl.ds(pl.multiple_of(at, 16), 16), :] = x[j]

    def regroup_first(k, c):
        for j in range(2):
            for v in range(3):
                regroup(v, 2 * k + j, 0, vis0_ref)
        return c

    lax.fori_loop(0, 2, regroup_first, 0)

    def values(v, s, vis_ref):
        return vis_ref[pl.ds(pl.multiple_of((v * BANDS + s) * GROUPS, GROUPS), GROUPS), :]

    def make_dft(i):
        k = 2 * (lax.broadcasted_iota(jnp.int32, (16, 256), 0) + 16 * i) + 1
        k = k * lax.broadcasted_iota(jnp.int32, (16, 256), 1) * 16
        for j, x in enumerate(cis_half(k)):
            rows = pl.ds(pl.multiple_of(128 * j + 16 * i, 16), 16)
            hi = x.astype(jnp.bfloat16)
            dft_ref[rows, 0:256] = hi
            dft_ref[rows, 256:512] = (x - hi.astype(jnp.float32)).astype(jnp.bfloat16)
            dft_ref[rows, 512:768] = hi

    def tables(s, vis_ref, p_ref, q_ref):
        off = values(2, s, vis_ref).astype(jnp.int32)
        col = off & (G - 1)
        row = off >> 12
        p_ref[pl.ds(16 * GROUPS, GROUPS), :] = (row & 15).astype(jnp.float32)
        p_ref[pl.ds(17 * GROUPS, GROUPS), :] = (row >> 4).astype(jnp.float32)
        half = cis_half(col)
        one = mul(half, half)
        base = mul((values(0, s, vis_ref), values(1, s, vis_ref)), cis_half(col * (2 * first + 15) - 16 * (row >> 4) - 256 * s))
        power = half
        for k in range(8):
            q_ref[pl.ds(k * SKIP, GROUPS), :] = power[0]
            q_ref[pl.ds((8 + k) * SKIP, GROUPS), :] = power[1]
            if k < 7:
                power = mul(power, one)
        step = one
        for k in range(4):
            step = mul(step, step)
        for k in range(8):
            p_ref[pl.ds(k * GROUPS, GROUPS), :] = base[0]
            p_ref[pl.ds((8 + k) * GROUPS, GROUPS), :] = base[1]
            if k < 7:
                base = mul(base, step)

    sub16 = lax.broadcasted_iota(jnp.int32, (16, 128), 0).astype(jnp.float32).astype(jnp.bfloat16)
    yes = jnp.ones((16, 128), jnp.bfloat16)
    no = jnp.zeros((16, 128), jnp.bfloat16)

    def made(g, p_ref, q_ref):
        def spread(row):
            return jnp.broadcast_to(p_ref[pl.ds(row * GROUPS + g, 1), :], (16, 128)).astype(jnp.bfloat16)

        high = jnp.where(spread(17) == sub16, spread(16), -yes)
        o = [jnp.where(high == jnp.bfloat16(k), yes, no) for k in range(16)]
        qr = q_ref[pl.ds(g, 8, stride=SKIP), :]
        qi = q_ref[pl.ds(8 * SKIP + g, 8, stride=SKIP), :]
        products = []
        for part, q in ((0, qr), (8, qi), (0, qi), (8, qr)):
            for k in range(0, 8, 2):
                two = [p_ref[pl.ds((part + k + j) * GROUPS + g, 1), :] * q for j in range(2)]
                products.append(jnp.concatenate(two).astype(jnp.bfloat16))
        return jnp.concatenate(o), jnp.concatenate(products)

    def phase(used, later, s, h_ref, vis_ref):
        tables(jnp.minimum(s + 1, BANDS - 1), vis_ref, *later)
        parts = [made(g, *used) for g in range(GROUPS)]
        o = jnp.concatenate([x[0] for x in parts], axis=1)
        e = jnp.concatenate([x[1] for x in parts], axis=1)
        part = lax.dot_general(o, e, (((1,), (1,)), ((), ())), preferred_element_type=jnp.float32)
        at = pl.ds(pl.multiple_of(s * 16, 16), 16)
        for k in range(16):
            h_ref[k, at, :] = part[16 * k : 16 * k + 16, :]

    sign = jnp.where(lax.broadcasted_iota(jnp.int32, (256, 128), 1) < 64, -1.0, 1.0)

    def dft(k, h_ref, y_ref):
        re, im = h_ref[k, :, 0:128], h_ref[k, :, 128:256]
        re = re + sign * pltpu.roll(re, 64, 1)
        im = im - sign * pltpu.roll(im, 64, 1)
        x = jnp.concatenate([re, im], axis=1)
        hi = x.astype(jnp.bfloat16)
        lo = (x - hi.astype(jnp.float32)).astype(jnp.bfloat16)
        both = jnp.concatenate([hi, hi, lo], axis=0)
        r = jnp.dot(dft_ref[...], both, preferred_element_type=jnp.float32)
        c_re, c_im, s_re, s_im = r[:128, :128], r[:128, 128:], r[128:, :128], r[128:, 128:]
        y_ref[k, 0:128, 0:128] = c_re - s_im
        y_ref[k, 0:128, 128:256] = c_im + s_re
        y_ref[k, 128:256, 0:128] = c_re + s_im
        y_ref[k, 128:256, 128:256] = c_im - s_re

    place = lax.broadcasted_iota(jnp.int32, (8, 128), 1)
    lower = place & 63
    lane = 2 * (lower - (lower & 7)) + jnp.where(place < 64, 8 + (lower & 7), 7 - (lower & 7))
    inner = place & 15
    source = ((place - inner) >> 1) + jnp.where(inner < 8, 71 - inner, inner - 8)
    lane = lane + first
    sub_row = lax.broadcasted_iota(jnp.int32, (8, 128), 0)
    scale = 0.5 / G
    y = (((lane + 2048) & 4095) - 2048).astype(jnp.float32) * scale
    rest = 1.0 - y * y
    def spread8(row, k):
        return jnp.broadcast_to(row[:, k : k + 1], (8, 128))

    w_row = sum(ref[384:385, :] for ref in own_refs) * 0.5
    taps_row = own_refs[0][385:386, :]

    def twiddles(line):
        tw = [None, cis_int(line)]
        for k in range(2, 16):
            tw.append(mul(tw[k // 2], tw[k - k // 2]))
        return tw

    def half_tile(t, half):
        line = sub_row + t * 8
        return pl.ds(pl.multiple_of(t * 8 + 128 * half, 8), 8), 255 - line if half else line

    def twist(at, k):
        return tw_ref[k - 1, at, :], tw_ref[14 + k, at, :]

    def terms(at, w, y_ref):
        xs = []
        for k in range(16):
            x = (y_ref[k, at, 0:128], y_ref[k, at, 128:256])
            xs.append(x if k == 0 else mul(x, twist(at, k)))
        f = fft(xs)
        result = []
        for j in range(16):
            turn = w * r_ref[j, at, :] - w
            turn = turn - jnp.round(turn)
            result.append(mul(f[j], cis4(turn)))
        return result

    taps = [spread8(taps_row, k) for k in range(8)]
    step = cis_int(lane)
    weight = [x.astype(jnp.bfloat16).astype(jnp.float32) * (1.0 / 512) for x in taps]
    b = (weight[7], jnp.zeros((8, 128), jnp.float32))
    for k in range(6, -1, -1):
        b = mul(b, step)
        b = (b[0] + weight[k], b[1])

    def prepare(t):
        for half in range(2):
            at, line = half_tile(t, half)
            tw = twiddles(line)
            for k in range(1, 16):
                tw_ref[k - 1, at, :] = tw[k][0]
                tw_ref[14 + k, at, :] = tw[k][1]
            ts = [(taps[0], jnp.zeros((8, 128), jnp.float32))]
            ts += [(tw[k][0] * taps[k], tw[k][1] * taps[k]) for k in range(1, 8)]
            a = fft(ts + [None] * 8)
            x0 = line.astype(jnp.float32) * scale
            for j in range(16):
                x = x0 + (256 * j if j < 8 else 256 * j - G) * scale
                z = rest - x * x
                r_ref[j, at, :] = z * lax.rsqrt(z)
                ab = mul(a[j], b)
                ab_ref[2 * j, at, :] = ab[0]
                ab_ref[2 * j + 1, at, :] = ab[1]

    buf0, buf1 = (p0_ref, q0_ref), (p1_ref, q1_ref)
    tables(0, vis0_ref, *buf0)

    def sets_of_first(i, c):
        for k in range(0, 4, 2):
            phase(buf0, buf1, 4 * i + k, h0_ref, vis0_ref)
            phase(buf1, buf0, 4 * i + k + 1, h0_ref, vis0_ref)
            make_dft(2 * i + k // 2)
            prepare(2 * i + k // 2)
        for v in range(3):
            regroup(v, i, 1, vis1_ref)
        return c

    lax.fori_loop(0, 4, sets_of_first, 0)
    tables(0, vis1_ref, *buf0)

    def sets_of_second(i, c):
        for k in range(0, 4, 2):
            phase(buf0, buf1, 4 * i + k, h1_ref, vis1_ref)
            dft(4 * i + k, h0_ref, y0_ref)
            phase(buf1, buf0, 4 * i + k + 1, h1_ref, vis1_ref)
            dft(4 * i + k + 1, h0_ref, y0_ref)
            prepare(8 + 2 * i + k // 2)
        return c

    lax.fori_loop(0, 4, sets_of_second, 0)
    w0 = spread8(w_row, 0)

    def tiles_of_first(i, c):
        for k in range(STEPS):
            dft(STEPS * i + k, h1_ref, y1_ref)
        for k in range(STEPS):
            for half in range(2):
                at, _ = half_tile(STEPS * i + k, half)
                for j, x in enumerate(terms(at, w0, y0_ref)):
                    sum_ref[j, at, 0:128] = x[0]
                    sum_ref[j, at, 128:256] = x[1]
        return c

    lax.fori_loop(0, 16 // STEPS, tiles_of_first, 0)
    w1 = spread8(w_row, 1)

    def tiles_of_second(t, c):
        for half in range(2):
            at, _ = half_tile(t, half)
            place = pl.ds(pl.multiple_of(248 - t * 8 if half else t * 8, 8), 8)
            for j, x in enumerate(terms(at, w1, y1_ref)):
                x = add(x, (sum_ref[j, at, 0:128], sum_ref[j, at, 128:256]))
                pixel = x[0] * ab_ref[2 * j, at, :] - x[1] * ab_ref[2 * j + 1, at, :]
                pixel = jnp.take_along_axis(pixel, source, axis=1)
                if half:
                    pixel = jnp.take_along_axis(pixel, 7 - sub_row, axis=0)
                out_ref[4 * (j // 2 % 4) + 2 * (j // 8) + j % 2, place, :] = pixel
        return c

    lax.fori_loop(0, 16, tiles_of_second, 0)


def part_image(first, *area, interpret=False):
    smem = pl.BlockSpec(memory_space=pltpu.SMEM)
    vmem = pl.BlockSpec(memory_space=pltpu.VMEM)
    return pl.pallas_call(
        image_kernel,
        out_shape=jax.ShapeDtypeStruct((16, 256, COLS), jnp.float32),
        in_specs=[smem] + [vmem] * 8,
        out_specs=vmem,
        scratch_shapes=[
            pltpu.VMEM((18 * GROUPS, 128), jnp.float32),
            pltpu.VMEM((18 * GROUPS, 128), jnp.float32),
            pltpu.VMEM((16 * SKIP, 128), jnp.float32),
            pltpu.VMEM((16 * SKIP, 128), jnp.float32),
            pltpu.VMEM((16, 256, 256), jnp.float32),
            pltpu.VMEM((16, 256, 256), jnp.float32),
            pltpu.VMEM((16, 256, 256), jnp.float32),
            pltpu.VMEM((16, 256, 256), jnp.float32),
            pltpu.VMEM((16, 256, 256), jnp.float32),
            pltpu.VMEM((256, 768), jnp.bfloat16),
            pltpu.VMEM((3 * BANDS * GROUPS, 128), jnp.float32),
            pltpu.VMEM((3 * BANDS * GROUPS, 128), jnp.float32),
            pltpu.VMEM((30, 256, 128), jnp.float32),
            pltpu.VMEM((16, 256, 128), jnp.float32),
            pltpu.VMEM((32, 256, 128), jnp.float32),
        ],
        compiler_params=pltpu.CompilerParams(vmem_limit_bytes=56 * 1024 * 1024),
        interpret=interpret,
    )(first, *area)


def shifted(x, axis, by):
    length = lax.axis_size(axis)
    return lax.ppermute(x, axis, [(i, (i + by) % length) for i in range(length)])


def local(visibility, target, offset, taps, w_plane):
    half = lax.axis_index("plane_0")
    out = buckets(target.reshape(1, 2048), offset.reshape(16, 128), visibility)
    own = lax.all_to_all(out, ("tile_1", "plane_1"), split_axis=0, concat_axis=0, tiled=True).reshape(384, 128)
    w_row = jnp.where(jnp.arange(128) == half, w_plane[0], 0.0)
    own = jnp.concatenate([own, w_row[None], jnp.pad(taps, (0, 120))[None], jnp.zeros((6, 128), jnp.float32)])
    area = [own] + [shifted(own, ("plane_0", "tile_0"), by) for by in (2, 1, 3)]
    area = area + [shifted(x, "tile_2", 1) for x in area]
    first = lax.axis_index(TILE) * 256 + half * COLS
    first = first.reshape(1).astype(jnp.int32)
    part = part_image(first, *area).reshape(G, COLS)
    arrived = lax.all_to_all(part, PLANE[::-1], split_axis=0, concat_axis=0, tiled=True)
    total = arrived.reshape(4, 2, 512, COLS).sum(axis=0)
    return jnp.concatenate([total[0], total[1]], axis=1)


def solution(mesh):
    finer = Mesh(
        mesh.devices.reshape(2, 4, 2, 4, 2), ("plane_0", "plane_1", "tile_0", "tile_1", "tile_2")
    )
    return jax.shard_map(
        local,
        mesh=finer,
        in_specs=(P(None, PLANE_TILE), P(PLANE_TILE, None), P(PLANE_TILE), P(), P(PLANE)),
        out_specs=P(PLANE, TILE),
        check_vma=False,
    )
```
